128 devices in a mesh: dp: 1, cp: 128 (over z, y, x, core).
Axes of the slice: x: 4, y: 4, z: 4, core: 2. Of those that a mesh axis runs over, the one named last changes fastest.
Arguments:
- x_in: bfloat16 [1, 8192, 16384], P('dp', 'cp')
- seg_ids: int32 [8192], P(('dp', 'cp'))
- positions: int32 [8192], P(('dp', 'cp'))
- attn_gain: bfloat16 [16384], replicated
- w_q: bfloat16 [16384, 2048], replicated
- w_k: bfloat16 [16384, 128], replicated
- w_v: bfloat16 [16384, 128], replicated
- w_o: bfloat16 [2048, 16384], replicated
- mlp_gain: bfloat16 [16384], replicated
- w_gate: bfloat16 [16384, 6656], replicated
- w_up: bfloat16 [16384, 6656], replicated
- w_down: bfloat16 [6656, 16384], replicated
Outputs:
- output 1: bfloat16 [1, 8192, 16384], P('dp', 'cp')
- output 2: bfloat16 [8192, 1, 128], P(('dp', 'cp'))
- output 3: bfloat16 [8192, 1, 128], P(('dp', 'cp'))
All inputs are finite; a program needn't handle non-finite values.
Results may differ from the reference program's by a relative error of at most 0.0125566.
Values are sent between devices in bfloat16 or wider.
A program may use at most 1.5 GiB of HBM per device.

```python
import jax
import jax.numpy as jnp
from jax import lax

MODEL_DIM = 16384
HEADS = 16
KV_HEADS = 1
HEAD_DIM = 128
FF_DIM = 6656
TOKENS_DEV = 64
CP_SIZE = 128
NUM_PROMPTS = 8
ATT_ROWS = 8

SEQ_LEN = TOKENS_DEV * CP_SIZE
CHUNK_ROWS = TOKENS_DEV // 2
GROUP_REP = HEADS // KV_HEADS
ROPE_THETA = 500000.0
ROPE_FACTOR = 8.0
LOW_FREQ = 1.0
HIGH_FREQ = 4.0
ORIG_CTX = 8192.0
NORM_EPS = 1e-5
NEG_BIG = -1e30


def rope_freqs():
    exponent = jnp.arange(0, HEAD_DIM, 2).astype(jnp.float32) / HEAD_DIM
    inv_freq = 1.0 / (ROPE_THETA ** exponent)
    wavelen = 2.0 * jnp.pi / inv_freq
    smooth = jnp.clip((ORIG_CTX / wavelen - LOW_FREQ) / (HIGH_FREQ - LOW_FREQ), 0.0, 1.0)
    return (1.0 - smooth) * inv_freq / ROPE_FACTOR + smooth * inv_freq


def apply_rope(tensor, cos_t, sin_t):
    half = tensor.shape[-1] // 2
    first = tensor[..., :half]
    second = tensor[..., half:]
    return jnp.concatenate([first * cos_t - second * sin_t, second * cos_t + first * sin_t], axis=-1)


def rms_norm(tensor, gain):
    vec_f32 = tensor.astype(jnp.float32)
    inv_rms = lax.rsqrt(jnp.mean(vec_f32 * vec_f32, axis=-1, keepdims=True) + NORM_EPS)
    return (vec_f32 * inv_rms * gain.astype(jnp.float32)).astype(jnp.bfloat16)


def project_rows(rows, pos_rows, attn_gain, w_q, w_k, w_v):
    count = rows.shape[0]
    normed = rms_norm(rows, attn_gain)
    angles = pos_rows.astype(jnp.float32)[:, None] * rope_freqs()[None, :]
    cos_t = jnp.cos(angles)[:, None, :]
    sin_t = jnp.sin(angles)[:, None, :]
    q_raw = jnp.dot(normed, w_q, preferred_element_type=jnp.float32).reshape(count, HEADS, HEAD_DIM)
    k_raw = jnp.dot(normed, w_k, preferred_element_type=jnp.float32).reshape(count, KV_HEADS, HEAD_DIM)
    v_raw = jnp.dot(normed, w_v, preferred_element_type=jnp.float32).reshape(count, KV_HEADS, HEAD_DIM)
    q_heads = apply_rope(q_raw, cos_t, sin_t).astype(jnp.bfloat16)
    k_heads = apply_rope(k_raw, cos_t, sin_t).astype(jnp.bfloat16)
    return q_heads, k_heads, v_raw.astype(jnp.bfloat16)


def attend_rows(block, k_all, v_all, seg_ids, positions):
    q_block, seg_rows, pos_rows = block
    q_grp = q_block.astype(jnp.float32).reshape(ATT_ROWS, KV_HEADS, GROUP_REP, HEAD_DIM)
    scores = jnp.einsum('qgrd,sgd->grqs', q_grp, k_all) * (HEAD_DIM ** -0.5)
    visible = (seg_ids[None, :] == seg_rows[:, None]) & (positions[None, :] <= pos_rows[:, None])
    scores = jnp.where(visible[None, None], scores, NEG_BIG)
    prob_w = jax.nn.softmax(scores, axis=-1)
    out_rows = jnp.einsum('grqs,sgd->qgrd', prob_w, v_all)
    return out_rows.reshape(ATT_ROWS, HEADS * HEAD_DIM).astype(jnp.bfloat16)


def finish_rows(rows, attn_rows, w_o, mlp_gain, w_gate, w_up, w_down):
    resid_mid = (rows.astype(jnp.float32) + jnp.dot(attn_rows, w_o, preferred_element_type=jnp.float32)).astype(jnp.bfloat16)
    normed = rms_norm(resid_mid, mlp_gain)
    gate = jnp.dot(normed, w_gate, preferred_element_type=jnp.float32)
    up_val = jnp.dot(normed, w_up, preferred_element_type=jnp.float32)
    hidden = (jax.nn.silu(gate) * up_val).astype(jnp.bfloat16)
    return (resid_mid.astype(jnp.float32) + jnp.dot(hidden, w_down, preferred_element_type=jnp.float32)).astype(jnp.bfloat16)


def mirror_order():
    row_idx = jnp.arange(SEQ_LEN)
    device = row_idx // TOKENS_DEV
    within = row_idx % TOKENS_DEV
    chunk_id = jnp.where(within < CHUNK_ROWS, device, 2 * CP_SIZE - 1 - device)
    return chunk_id * CHUNK_ROWS + within % CHUNK_ROWS


def draw_layout(key):
    key_long, key_cuts = jax.random.split(key)
    long_len = SEQ_LEN // 2 + jax.random.randint(key_long, (), 0, SEQ_LEN // 4 + 1)
    cuts = jnp.sort(jax.random.randint(key_cuts, (NUM_PROMPTS - 2,), long_len, SEQ_LEN))
    bounds = jnp.concatenate([long_len[None], cuts]).astype(jnp.int32)
    token = jnp.arange(SEQ_LEN, dtype=jnp.int32)
    after = token[:, None] >= bounds[None, :]
    seg_nat = jnp.sum(after, axis=1).astype(jnp.int32)
    start = jnp.max(jnp.where(after, bounds[None, :], 0), axis=1)
    pos_nat = (token - start).astype(jnp.int32)
    order = mirror_order()
    return seg_nat[order], pos_nat[order]


def normal_weight(key, shape, scale):
    return (scale * jax.random.normal(key, shape, jnp.float32)).astype(jnp.bfloat16)


def setup_inputs(seed: int = 0, part: int = 0) -> dict:
    root = jax.random.key(seed)
    shared = jax.random.split(root, 10)
    part_keys = jax.random.split(jax.random.fold_in(root, part), 2)
    seg_ids, positions = draw_layout(part_keys[0])
    x_in = normal_weight(part_keys[1], (1, SEQ_LEN, MODEL_DIM), 0.5)
    attn_gain = (1.0 + 0.3 * jax.random.normal(shared[0], (MODEL_DIM,), jnp.float32)).astype(jnp.bfloat16)
    w_q = normal_weight(shared[1], (MODEL_DIM, HEADS * HEAD_DIM), 1.5 * MODEL_DIM ** -0.5)
    w_k = normal_weight(shared[2], (MODEL_DIM, KV_HEADS * HEAD_DIM), 1.5 * MODEL_DIM ** -0.5)
    w_v = normal_weight(shared[3], (MODEL_DIM, KV_HEADS * HEAD_DIM), MODEL_DIM ** -0.5)
    w_o = normal_weight(shared[4], (HEADS * HEAD_DIM, MODEL_DIM), 2.0 * (HEADS * HEAD_DIM) ** -0.5)
    mlp_gain = (1.0 + 0.3 * jax.random.normal(shared[5], (MODEL_DIM,), jnp.float32)).astype(jnp.bfloat16)
    w_gate = normal_weight(shared[6], (MODEL_DIM, FF_DIM), MODEL_DIM ** -0.5)
    w_up = normal_weight(shared[7], (MODEL_DIM, FF_DIM), MODEL_DIM ** -0.5)
    w_down = normal_weight(shared[8], (FF_DIM, MODEL_DIM), FF_DIM ** -0.5)
    return {'x_in': x_in, 'seg_ids': seg_ids, 'positions': positions, 'attn_gain': attn_gain, 'w_q': w_q, 'w_k': w_k, 'w_v': w_v, 'w_o': w_o, 'mlp_gain': mlp_gain, 'w_gate': w_gate, 'w_up': w_up, 'w_down': w_down}


def reference(x_in, seg_ids, positions, attn_gain, w_q, w_k, w_v, w_o, mlp_gain, w_gate, w_up, w_down):
    num_blocks = SEQ_LEN // CHUNK_ROWS
    row_blocks = x_in.reshape(num_blocks, CHUNK_ROWS, MODEL_DIM)
    pos_blocks = positions.reshape(num_blocks, CHUNK_ROWS)
    q_heads, k_heads, v_heads = lax.map(lambda block: project_rows(block[0], block[1], attn_gain, w_q, w_k, w_v), (row_blocks, pos_blocks))
    k_cache = k_heads.reshape(SEQ_LEN, KV_HEADS, HEAD_DIM)
    v_cache = v_heads.reshape(SEQ_LEN, KV_HEADS, HEAD_DIM)
    k_all = k_cache.astype(jnp.float32)
    v_all = v_cache.astype(jnp.float32)
    q_rows = q_heads.reshape(SEQ_LEN // ATT_ROWS, ATT_ROWS, HEADS, HEAD_DIM)
    seg_rows = seg_ids.reshape(SEQ_LEN // ATT_ROWS, ATT_ROWS)
    pos_rows = positions.reshape(SEQ_LEN // ATT_ROWS, ATT_ROWS)
    attn_rows = lax.map(lambda block: attend_rows(block, k_all, v_all, seg_ids, positions), (q_rows, seg_rows, pos_rows))
    attn_blocks = attn_rows.reshape(num_blocks, CHUNK_ROWS, HEADS * HEAD_DIM)
    z_blocks = lax.map(lambda block: finish_rows(block[0], block[1], w_o, mlp_gain, w_gate, w_up, w_down), (row_blocks, attn_blocks))
    return z_blocks.reshape(1, SEQ_LEN, MODEL_DIM), k_cache, v_cache
```

```python
import functools
import math

import jax
import jax.numpy as jnp
from jax import lax
from jax.experimental import pallas as pl
from jax.experimental.pallas import tpu as pltpu
from jax.sharding import PartitionSpec as P

MODEL = 16384
HALF = MODEL // 2
HEADS = 16
HEAD_DIM = 128
QCOLS = HEADS * HEAD_DIM // 2
FF = 6656
FFH = FF // 2
ROWS = 64
CHUNK = 32
PAIR = 2 * ROWS
SEQ = 8192
ROPE_THETA = 500000.0
ROPE_FACTOR = 8.0
LOW_FREQ = 1.0
HIGH_FREQ = 4.0
ORIG_CTX = 8192.0
NORM_EPS = 1e-5
NEG_BIG = -1e30
EXP_SCALE = HEAD_DIM ** -0.5 * math.log2(math.e)

N1 = 5
N2 = 10
KC = 512
NB = 2048
Q_TRIPS = MODEL // (2 * KC)
O_TRIPS = (HALF // NB) * (HEADS * HEAD_DIM // KC)
D_K = FF // KC
D_TRIPS = (HALF // NB) * D_K
G_TRIPS = MODEL // KC
KV_PER_SLOT = FFH // 256
KV_PIECES = MODEL // KC
HOOK_B, HOOK_C = 5, 13

MESH = pl.DeviceIdType.MESH
F32 = jnp.float32
BF16 = jnp.bfloat16
BLOCKS = ((0, 0, 'yzx'), (1, 0, 'zxy'), (0, 1, 'xyz'), (1, 1, 'xyz'))


def rope_tables(pos, lanes=HEAD_DIM):
    lane = lax.broadcasted_iota(jnp.int32, (8, lanes), 1)
    j = lax.rem(lane, HEAD_DIM // 2).astype(F32)
    inv_freq = jnp.exp(j * (-2.0 / HEAD_DIM * math.log(ROPE_THETA)))
    wavelen = (2.0 * math.pi) / inv_freq
    smooth = jnp.clip((ORIG_CTX / wavelen - LOW_FREQ) / (HIGH_FREQ - LOW_FREQ), 0.0, 1.0)
    freq = ((1.0 - smooth) * inv_freq / ROPE_FACTOR + smooth * inv_freq)[0:1]
    angle = pos * freq
    sign = jnp.where(lane[0:1] < HEAD_DIM // 2, -1.0, 1.0)
    return jnp.cos(angle), jnp.sin(angle) * sign


def rope(t, cos_t, sin_t):
    return t * cos_t + pltpu.roll(t, HEAD_DIM // 2, 1) * sin_t


def layer_kernel(x_hbm, pos_ref, ag_ref, wq, wk, wv, wo, mg_ref, wg, wu, wd,
                 z_hbm, k_out, v_out,
                 x128, bbuf, kv, w1, w2, acc, acc_g, acc_u, qs, att, ml, obuf, mbuf, st, ss, zst, kst,
                 xl_sem, xs_sem, xr_sem, sts_sem, str_sem, kvw_sem, w1_sem, w2_sem, gs_sem, gr_sem, fs_sem, fr_sem,
                 os_sem, or_sem, sss_sem, ssr_sem, bs_sem, br_sem, ms_sem, mr_sem, zl_sem, zs_sem, zr_sem, ko_sem):
    me = lax.axis_index('cp')
    core = lax.rem(me, 2)
    chip = lax.div(me, 2)
    coords = {'x': lax.rem(chip, 4), 'y': lax.rem(lax.div(chip, 4), 4), 'z': lax.div(chip, 16)}
    sib = me + 1 - 2 * core
    other = 1 - core

    def peer(dim, k):
        c = dict(coords)
        c[dim] = lax.rem(c[dim] + k, 4)
        return ((c['z'] * 4 + c['y']) * 4 + c['x']) * 2 + core

    def remote(src, dst, s, r, dev):
        return pltpu.make_async_remote_copy(src, dst, s, r, device_id={'cp': dev}, device_id_type=MESH)

    def to_sib(src, dst, s, r):
        return remote(src, dst, s, r, sib)

    own_rows = pl.ds(pl.multiple_of(core * ROWS, ROWS), ROWS)
    sib_rows = pl.ds(pl.multiple_of(other * ROWS, ROWS), ROWS)
    own_half = pl.multiple_of(core * HALF, HALF)
    sib_half = pl.multiple_of(other * HALF, HALF)

    def kv_dst(c, width):
        return w1.at[lax.div(c, KV_PER_SLOT), :, pl.ds(pl.multiple_of(lax.rem(c, KV_PER_SLOT) * 256 + (128 if width == -128 else 0), 128), abs(width))]

    def kv_start(c):
        rows = pl.ds(pl.multiple_of(c * KC, KC), KC)
        pltpu.make_async_copy(wk.at[rows, :], kv_dst(c, 128), kvw_sem.at[c]).start()
        pltpu.make_async_copy(wv.at[rows, :], kv_dst(c, -128), kvw_sem.at[c]).start()

    def kv_wait(c):
        pltpu.make_async_copy(wq.at[pl.ds(0, KC), pl.ds(0, 256)], kv_dst(c, 256), kvw_sem.at[c]).wait()

    def w2_start(n):
        slot = lax.rem(n, N2)

        @pl.when(n < Q_TRIPS)
        def _():
            for h in range(2):
                rows = pl.ds(pl.multiple_of(n * (2 * KC) + h * KC, KC), KC)
                cols = pl.ds(pl.multiple_of(core * QCOLS, QCOLS), QCOLS)
                pltpu.make_async_copy(wq.at[rows, cols], w2.at[slot, :, pl.ds(h * QCOLS, QCOLS)], w2_sem.at[slot]).start()

        @pl.when((n >= Q_TRIPS) & (n < Q_TRIPS + O_TRIPS))
        def _():
            rows = pl.ds(pl.multiple_of(o_chunk(n - Q_TRIPS) * KC, KC), KC)
            cols = pl.ds(pl.multiple_of(own_half + lax.div(n - Q_TRIPS, 4) * NB, NB), NB)
            pltpu.make_async_copy(wo.at[rows, cols], w2.at[slot], w2_sem.at[slot]).start()

        @pl.when((n >= Q_TRIPS + O_TRIPS) & (n < Q_TRIPS + O_TRIPS + D_TRIPS))
        def _():
            i = n - (Q_TRIPS + O_TRIPS)
            rows = pl.ds(pl.multiple_of(d_chunk(lax.rem(i, D_K)) * KC, KC), KC)
            cols = pl.ds(pl.multiple_of(own_half + lax.div(i, D_K) * NB, NB), NB)
            pltpu.make_async_copy(wd.at[rows, cols], w2.at[slot], w2_sem.at[slot]).start()

    def w2_wait(n):
        slot = lax.rem(n, N2)
        pltpu.make_async_copy(wo.at[pl.ds(0, KC), pl.ds(0, NB)], w2.at[slot], w2_sem.at[slot]).wait()
        return slot

    def o_chunk(i):
        kk = lax.rem(i, 4)
        return lax.rem(kk + 2 * core, 4)

    def d_chunk(kk):
        late = jnp.where(kk < 6, kk + 7, jnp.where(kk == 6, 6, kk - 7))
        return jnp.where(core == 0, kk, late)

    def g_chunk(i):
        return lax.rem(i + core * (G_TRIPS // 2), G_TRIPS)

    def w1_start(n):
        slot = lax.rem(n, N1)
        rows = pl.ds(pl.multiple_of(g_chunk(lax.div(n, 2)) * KC, KC), KC)
        cols = pl.ds(pl.multiple_of(core * FFH, FFH), FFH)

        @pl.when((n < 2 * G_TRIPS) & (lax.rem(n, 2) == 0))
        def _():
            pltpu.make_async_copy(wg.at[rows, cols], w1.at[slot], w1_sem.at[slot]).start()

        @pl.when((n < 2 * G_TRIPS) & (lax.rem(n, 2) == 1))
        def _():
            pltpu.make_async_copy(wu.at[rows, cols], w1.at[slot], w1_sem.at[slot]).start()

    def w1_wait(n):
        slot = lax.rem(n, N1)
        pltpu.make_async_copy(wg.at[pl.ds(0, KC), pl.ds(0, FFH)], w1.at[slot], w1_sem.at[slot]).wait()
        return slot

    x_local = pltpu.make_async_copy(x_hbm, x128.at[own_rows, :], xl_sem)
    x_local.start()

    @pl.loop(0, KV_PIECES)
    def _(c):
        kv_start(c)

    @pl.loop(0, N2)
    def _(n):
        w2_start(n)

    barrier = pltpu.get_barrier_semaphore()
    pl.semaphore_signal(barrier, inc=1, device_id={'cp': sib}, device_id_type=MESH)
    for dim in 'xyz':
        for k in (1, 2, 3):
            pl.semaphore_signal(barrier, inc=1, device_id={'cp': peer(dim, k)}, device_id_type=MESH)
    pl.semaphore_wait(barrier, 10)

    XP = 4

    def x_copy(i):
        cols = pl.ds(i * (MODEL // XP), MODEL // XP)
        return to_sib(x_hbm.at[:, cols], x128.at[own_rows, cols], xs_sem.at[i], xr_sem.at[i])

    for i in range(XP):
        x_copy(i).start()

    x_local.wait()

    def square_sum(i, part):
        for u in range(8):
            v = x128[own_rows, pl.ds(pl.multiple_of(i * 1024 + u * 128, 128), 128)].astype(F32)
            part = part + v * v
        return part

    part = lax.fori_loop(0, MODEL // 1024, square_sum, jnp.zeros((ROWS, 128), F32))
    inv_own = lax.rsqrt(jnp.sum(part, axis=1, keepdims=True) / MODEL + NORM_EPS)
    eye = lax.broadcasted_iota(jnp.int32, (ROWS, ROWS), 0) == lax.broadcasted_iota(jnp.int32, (ROWS, ROWS), 1)
    pos_own = jnp.sum(jnp.where(eye, jnp.broadcast_to(pos_ref[...].astype(F32), (ROWS, ROWS)), 0.0), axis=1, keepdims=True)
    lane = lax.broadcasted_iota(jnp.int32, (ROWS, 128), 1)
    st[core] = jnp.where(lane == 0, inv_own, pos_own)
    st_copy = to_sib(st.at[core], st.at[core], sts_sem, str_sem)
    st_copy.start()

    def normalize(rows, inv, lo, hi):
        @pl.loop(lo, hi)
        def _(i):
            for u in range(4):
                cols = pl.ds(pl.multiple_of(i * 1024 + u * 256, 256), 256)
                v = x128[rows, cols].astype(F32) * inv * ag_ref[:, cols].astype(F32)
                bbuf[rows, cols] = v.astype(BF16)

    normalize(own_rows, inv_own, 0, MODEL // 1024)

    def kv_trip(i, total):
        for u in range(8):
            kv_wait(i * 8 + u)
        for u in range(8):
            c = i * 8 + u
            w = w1[lax.div(c, KV_PER_SLOT), :, pl.ds(pl.multiple_of(lax.rem(c, KV_PER_SLOT) * 256, 256), 256)]
            a = bbuf[own_rows, pl.ds(pl.multiple_of(c * KC, KC), KC)]
            total = total + jnp.dot(a, w, preferred_element_type=F32)
        return total

    kv_raw = lax.fori_loop(0, KV_PIECES // 8, kv_trip, jnp.zeros((ROWS, 256), F32))
    cos_own, sin_own = rope_tables(pos_own)
    k_own = rope(kv_raw[:, :128], cos_own, sin_own).astype(BF16)
    v_own = kv_raw[:, 128:].astype(BF16)
    kst[0] = k_own
    kst[1] = v_own
    r0 = (pl.multiple_of(core * CHUNK, CHUNK), pl.multiple_of(other * CHUNK, CHUNK))
    cx, cy, cz = coords['x'], coords['y'], coords['z']
    for i, t in enumerate((k_own, v_own)):
        kv[i, 0, cz, cy, cx, pl.ds(r0[0], CHUNK), :] = t[:CHUNK]
        kv[i, 1, cz, cy, cx, pl.ds(r0[1], CHUNK), :] = t[CHUNK:]
    k_store = pltpu.make_async_copy(kst.at[0], k_out, ko_sem.at[0])
    v_store = pltpu.make_async_copy(kst.at[1], v_out, ko_sem.at[1])
    k_store.start()
    v_store.start()

    def piece(b, pos, full):
        i, half, _ = BLOCKS[b]
        idx = [slice(None) if d in full else pos[d] for d in 'zyx']
        return kv.at[(i, half, *idx, pl.ds(r0[half], CHUNK), slice(None))]

    def from_peer(b, ph, k):
        dims = BLOCKS[b][2]
        pos = dict(coords)
        pos[dims[ph]] = lax.rem(pos[dims[ph]] + 4 - k, 4)
        return piece(b, pos, dims[:ph])

    def guarded(b, ph, k, side, action):
        if ph == 2 and BLOCKS[b][1] == 1:
            pl.when(cz + k >= 4 if side == 'send' else cz < k)(action)
        else:
            action()

    def gather_copy(b, ph, k):
        dims = BLOCKS[b][2]
        src = piece(b, coords, dims[:ph])
        return remote(src, src, gs_sem.at[b, ph, k - 1], gr_sem.at[b, ph, k - 1], peer(dims[ph], k))

    def own_forward(b):
        src = piece(b, coords, '')
        return to_sib(src, src, fs_sem.at[b, 9], fr_sem.at[b, 9])

    def sib_own(b):
        i, half, _ = BLOCKS[b]
        dst = kv.at[i, half, cz, cy, cx, pl.ds(r0[1 - half], CHUNK), :]
        return to_sib(dst, dst, fs_sem.at[b, 9], fr_sem.at[b, 9])

    def forward(b, ph, k):
        src = from_peer(b, ph, k)
        return to_sib(src, src, fs_sem.at[b, ph * 3 + k - 1], fr_sem.at[b, ph * 3 + k - 1])

    def phase_start(ph):
        for b in range(4):
            for k in (1, 2, 3):
                guarded(b, ph, k, 'send', lambda b=b, k=k: gather_copy(b, ph, k).start())

    def phase_finish(ph):
        for b in range(4):
            for k in (1, 2, 3):
                def got(b=b, k=k):
                    gather_copy(b, ph, k).wait_recv()
                    forward(b, ph, k).start()
                guarded(b, ph, k, 'recv', got)
        for b in range(4):
            for k in (1, 2, 3):
                guarded(b, ph, k, 'send', lambda b=b, k=k: gather_copy(b, ph, k).wait_send())

    phase_start(0)
    for b in range(4):
        own_forward(b).start()

    st_copy.wait()
    inv_sib = st[other][:, 0:1]
    for i in range(XP):
        x_copy(i).wait()
        normalize(sib_rows, inv_sib, i * 4, i * 4 + 4)

    acc[...] = jnp.zeros_like(acc)

    @pl.loop(0, Q_TRIPS)
    def _(i):
        @pl.when(i == HOOK_B)
        def _():
            phase_finish(0)
            phase_start(1)

        @pl.when(i == HOOK_C)
        def _():
            phase_finish(1)
            phase_start(2)

        slot = w2_wait(i)
        k0 = pl.multiple_of(i * (2 * KC), 2 * KC)
        acc[:, :QCOLS] += (jnp.dot(bbuf[:, pl.ds(k0, KC)], w2[slot, :, :QCOLS], preferred_element_type=F32)
                           + jnp.dot(bbuf[:, pl.ds(k0 + KC, KC)], w2[slot, :, QCOLS:], preferred_element_type=F32))
        w2_start(i + N2)

    @pl.loop(0, N1)
    def _(n):
        w1_start(n)

    pos_all = jnp.concatenate([st[0][:, 1:2], st[1][:, 1:2]], axis=0)
    cos_t, sin_t = rope_tables(pos_all)
    for h in range(HEADS // 2):
        q = rope(acc[:, h * 128:(h + 1) * 128], cos_t, sin_t).astype(BF16)
        qs[0, h, :CHUNK] = q[:32]
        qs[0, h, CHUNK:] = q[64:96]
        qs[1, h, :CHUNK] = q[96:]
        qs[1, h, CHUNK:] = q[32:64]

    phase_finish(2)
    for b in range(4):
        own_forward(b).wait_send()
        sib_own(b).wait_recv()
    for ph in range(3):
        for b in range(4):
            for k in (1, 2, 3):
                def passed(b=b, ph=ph, k=k):
                    forward(b, ph, k).wait_send()
                    sib_piece(b, ph, k).wait_recv()

                def sib_piece(b, ph, k):
                    i, half, dims = BLOCKS[b]
                    pos = dict(coords)
                    pos[dims[ph]] = lax.rem(pos[dims[ph]] + 4 - k, 4)
                    idx = [slice(None) if d in dims[:ph] else pos[d] for d in 'zyx']
                    dst = kv.at[(i, half, *idx, pl.ds(r0[1 - half], CHUNK), slice(None))]
                    return to_sib(dst, dst, fs_sem.at[b, ph * 3 + k - 1], fr_sem.at[b, ph * 3 + k - 1])
                guarded(b, ph, k, 'recv', passed)

    ml[:, 0] = jnp.full((2, 512, 128), NEG_BIG, F32)
    ml[:, 1] = jnp.zeros((2, 512, 128), F32)
    att[...] = jnp.zeros_like(att)
    c8 = lax.div(chip, 8)

    @pl.loop(0, 17)
    def _(s):
        late_q = s > c8
        late_k = late_q & (s < 9)
        t = jnp.where(late_q, jnp.where(late_k, s - 1, s - 9), c8 - s)
        qh = late_q.astype(jnp.int32)
        kh = late_k.astype(jnp.int32)
        tz, ty = lax.div(t, 2), lax.rem(t, 2) * 2
        keys = kv[0, kh, tz, pl.ds(ty, 2)].reshape(512, 128)
        vals = kv[1, kh, tz, pl.ds(ty, 2)].reshape(512, 128)
        q = qs[qh].reshape(512, 128)
        scores = lax.dot_general(q, keys, (((1,), (1,)), ((), ())), preferred_element_type=F32)
        u = lax.broadcasted_iota(jnp.int32, (1, 512), 1)
        back = lax.div(u, 64)
        key_nat = jnp.where(late_k, SEQ - 64 * (8 * t + 1) - 128 * back + u, 512 * t + u)
        row = lax.broadcasted_iota(jnp.int32, (64, 1), 0)
        row_nat = jnp.where(late_q, SEQ - 64 * (chip + 1), 64 * chip) + row
        pos_e = jnp.concatenate([st[0][:32, 1:2], st[1][:32, 1:2]], axis=0)
        pos_l = jnp.concatenate([st[1][32:, 1:2], st[0][32:, 1:2]], axis=0)
        row_first = row_nat - jnp.where(late_q, pos_l, pos_e).astype(jnp.int32)
        visible = (key_nat >= row_first) & (key_nat <= row_nat)
        scores = jnp.where(visible[None], scores.reshape(8, 64, 512), NEG_BIG).reshape(512, 512)
        m_old = ml[qh, 0]
        m_new = jnp.maximum(m_old, jnp.max(scores, axis=1, keepdims=True))
        p = jnp.exp2((scores - m_new[:, :1]) * EXP_SCALE)
        alpha = jnp.exp2((m_old - m_new) * EXP_SCALE)
        ml[qh, 0] = m_new
        ml[qh, 1] = ml[qh, 1] * alpha + jnp.sum(p, axis=1, keepdims=True)
        att[qh] = att[qh] * alpha + jnp.dot(p.astype(BF16), vals, preferred_element_type=F32)

    for h in range(HEADS // 2):
        r = slice(h * 64, (h + 1) * 64)
        cols = slice(h * 128, (h + 1) * 128)
        o_e = (att[0, r] / ml[0, 1, r]).astype(BF16)
        o_l = (att[1, r] / ml[1, 1, r]).astype(BF16)
        obuf[core, 0:32, cols] = o_e[:32]
        obuf[core, 64:96, cols] = o_e[32:]
        obuf[core, 96:128, cols] = o_l[:32]
        obuf[core, 32:64, cols] = o_l[32:]
    o_copy = to_sib(obuf.at[core], obuf.at[core], os_sem, or_sem)
    o_copy.start()

    ss[core] = jnp.zeros((PAIR, 128), F32)
    acc[...] = jnp.zeros_like(acc)

    @pl.loop(0, O_TRIPS)
    def _(i):
        @pl.when(i == 2)
        def _():
            o_copy.wait()

        slot = w2_wait(Q_TRIPS + i)
        ch = o_chunk(i)
        a = obuf[lax.div(ch, 2), :, pl.ds(pl.multiple_of(lax.rem(ch, 2) * KC, KC), KC)]
        acc[...] += jnp.dot(a, w2[slot], preferred_element_type=F32)
        w2_start(Q_TRIPS + i + N2)

        @pl.when(lax.rem(i, 4) == 3)
        def _():
            n = lax.div(i, 4)

            def column(j, part):
                cols = pl.ds(pl.multiple_of(own_half + n * NB + j * 128, 128), 128)
                local = pl.ds(pl.multiple_of(j * 128, 128), 128)
                h = (x128[:, cols].astype(F32) + acc[:, local]).astype(BF16)
                x128[:, cols] = h
                acc[:, local] = jnp.zeros((PAIR, 128), F32)
                hf = h.astype(F32)
                return part + hf * hf

            ss[core] += lax.fori_loop(0, NB // 128, column, jnp.zeros((PAIR, 128), F32))

    ss_copy = to_sib(ss.at[core], ss.at[core], sss_sem, ssr_sem)
    ss_copy.start()
    ss_copy.wait()
    inv_h = lax.rsqrt(jnp.sum(ss[0] + ss[1], axis=1, keepdims=True) / MODEL + NORM_EPS)

    BP = HALF // NB

    def b_copy(i):
        cols = pl.ds(pl.multiple_of(own_half + i * NB, NB), NB)
        return to_sib(bbuf.at[:, cols], bbuf.at[:, cols], bs_sem.at[i], br_sem.at[i])

    def b_arrival(i):
        cols = pl.ds(pl.multiple_of(sib_half + i * NB, NB), NB)
        return to_sib(bbuf.at[:, cols], bbuf.at[:, cols], bs_sem.at[i], br_sem.at[i])

    for i in range(BP):
        @pl.loop(0, NB // 256)
        def _(j):
            cols = pl.ds(pl.multiple_of(own_half + i * NB + j * 256, 256), 256)
            bbuf[:, cols] = (x128[:, cols].astype(F32) * inv_h * mg_ref[:, cols].astype(F32)).astype(BF16)
        b_copy(i).start()

    acc_g[...] = jnp.zeros_like(acc_g)
    acc_u[...] = jnp.zeros_like(acc_u)

    @pl.loop(0, G_TRIPS)
    def _(i):
        for q in range(BP):
            @pl.when(i == G_TRIPS // 2 + q * (NB // KC))
            def _():
                b_arrival(q).wait_recv()

        a = bbuf[:, pl.ds(pl.multiple_of(g_chunk(i) * KC, KC), KC)]
        sg = w1_wait(2 * i)
        acc_g[...] += jnp.dot(a, w1[sg], preferred_element_type=F32)
        w1_start(2 * i + N1)
        su = w1_wait(2 * i + 1)
        acc_u[...] += jnp.dot(a, w1[su], preferred_element_type=F32)
        w1_start(2 * i + 1 + N1)

    @pl.loop(0, FFH // 256)
    def _(j):
        local = pl.ds(pl.multiple_of(j * 256, 256), 256)
        g = acc_g[:, local]
        m = g * (1.0 / (1.0 + jnp.exp(-g))) * acc_u[:, local]
        mbuf[:, pl.ds(pl.multiple_of(core * FFH + j * 256, 256), 256)] = m.astype(BF16)

    m_cols = pl.ds(pl.multiple_of(core * FFH, FFH), FFH)
    m_copy = to_sib(mbuf.at[:, m_cols], mbuf.at[:, m_cols], ms_sem, mr_sem)
    m_copy.start()

    acc[...] = jnp.zeros_like(acc)

    def z_cols(n):
        return pl.ds(pl.multiple_of(own_half + n * NB, NB), NB)

    def z_local(n):
        return pltpu.make_async_copy(zst.at[lax.rem(n, 2), own_rows, :], z_hbm.at[:, z_cols(n)], zl_sem.at[lax.rem(n, 2)])

    def z_remote(n):
        return to_sib(zst.at[lax.rem(n, 2), sib_rows, :], z_hbm.at[:, z_cols(n)], zs_sem.at[lax.rem(n, 2)], zr_sem.at[n])

    def z_arrival(n):
        cols = pl.ds(pl.multiple_of(sib_half + n * NB, NB), NB)
        return to_sib(zst.at[lax.rem(n, 2), sib_rows, :], z_hbm.at[:, cols], zs_sem.at[lax.rem(n, 2)], zr_sem.at[n])

    @pl.loop(0, D_TRIPS)
    def _(i):
        @pl.when(i == 6)
        def _():
            m_copy.wait()

        n, kk = lax.div(i, D_K), lax.rem(i, D_K)
        slot = w2_wait(Q_TRIPS + O_TRIPS + i)
        a = mbuf[:, pl.ds(pl.multiple_of(d_chunk(kk) * KC, KC), KC)]
        acc[...] += jnp.dot(a, w2[slot], preferred_element_type=F32)
        w2_start(Q_TRIPS + O_TRIPS + i + N2)

        @pl.when(kk == D_K - 1)
        def _():
            @pl.when(n >= 2)
            def _():
                z_local(n - 2).wait()
                z_remote(n - 2).wait_send()

            zslot = lax.rem(n, 2)

            @pl.loop(0, NB // 256)
            def _(j):
                cols = pl.ds(pl.multiple_of(own_half + n * NB + j * 256, 256), 256)
                local = pl.ds(pl.multiple_of(j * 256, 256), 256)
                zst[zslot, :, local] = (x128[:, cols].astype(F32) + acc[:, local]).astype(BF16)
                acc[:, local] = jnp.zeros((PAIR, 256), F32)

            z_local(n).start()
            z_remote(n).start()

    for n in range(HALF // NB):
        if n >= HALF // NB - 2:
            z_local(n).wait()
            z_remote(n).wait_send()
        z_arrival(n).wait_recv()
        b_copy(n).wait_send()
    k_store.wait()
    v_store.wait()


def solution(mesh):
    def device_fn(x_loc, seg_loc, pos_loc, attn_gain, w_q, w_k, w_v, w_o, mlp_gain, w_gate, w_up, w_down):
        any_space = pl.BlockSpec(memory_space=pl.ANY)
        vmem = pl.BlockSpec(memory_space=pltpu.VMEM)
        dma = pltpu.SemaphoreType.DMA
        z_rows, k_rows, v_rows = pl.pallas_call(
            layer_kernel,
            out_shape=(jax.ShapeDtypeStruct((ROWS, MODEL), BF16), jax.ShapeDtypeStruct((ROWS, HEAD_DIM), BF16), jax.ShapeDtypeStruct((ROWS, HEAD_DIM), BF16)),
            in_specs=[any_space, vmem, vmem, any_space, any_space, any_space, any_space, vmem, any_space, any_space, any_space],
            out_specs=(any_space, any_space, any_space),
            scratch_shapes=[
                pltpu.VMEM((PAIR, MODEL), BF16),
                pltpu.VMEM((PAIR, MODEL), BF16),
                pltpu.VMEM((2, 2, 4, 4, 4, 64, 128), BF16),
                pltpu.VMEM((N1, KC, FFH), BF16),
                pltpu.VMEM((N2, KC, NB), BF16),
                pltpu.VMEM((PAIR, NB), F32),
                pltpu.VMEM((PAIR, FFH), F32),
                pltpu.VMEM((PAIR, FFH), F32),
                pltpu.VMEM((2, HEADS // 2, 64, 128), BF16),
                pltpu.VMEM((2, 512, 128), F32),
                pltpu.VMEM((2, 2, 512, 128), F32),
                pltpu.VMEM((2, PAIR, QCOLS), BF16),
                pltpu.VMEM((PAIR, FF), BF16),
                pltpu.VMEM((2, ROWS, 128), F32),
                pltpu.VMEM((2, PAIR, 128), F32),
                pltpu.VMEM((2, PAIR, NB), BF16),
                pltpu.VMEM((2, ROWS, 128), BF16),
                dma, dma((4,)), dma((4,)), dma, dma, dma((KV_PIECES,)), dma((N1,)), dma((N2,)),
                dma((4, 3, 3)), dma((4, 3, 3)), dma((4, 10)), dma((4, 10)),
                dma, dma, dma, dma, dma((4,)), dma((4,)), dma, dma, dma((2,)), dma((2,)), dma((4,)), dma((2,)),
            ],
            compiler_params=pltpu.CompilerParams(collective_id=0, has_side_effects=True, vmem_limit_bytes=67043328),
            name='layer',
        )(x_loc[0], pos_loc.reshape(1, ROWS), attn_gain.reshape(1, MODEL), w_q, w_k, w_v, w_o, mlp_gain.reshape(1, MODEL), w_gate, w_up, w_down)
        return z_rows[None], k_rows[:, None, :], v_rows[:, None, :]

    seq_spec = P(('dp', 'cp'))
    return jax.shard_map(device_fn, mesh=mesh, in_specs=(P('dp', 'cp', None), seq_spec, seq_spec, P(), P(), P(), P(), P(), P(), P(), P(), P()), out_specs=(P('dp', 'cp', None), P(('dp', 'cp'), None, None), P(('dp', 'cp'), None, None)), check_vma=False)
```

```python
import functools
import math

import jax
import jax.numpy as jnp
from jax import lax
from jax.experimental import pallas as pl
from jax.experimental.pallas import tpu as pltpu
from jax.sharding import PartitionSpec as P

LANES = 128
SUBLANES = 8
SIDE = 4
MODEL = 16384
HALF = MODEL // 2
HEADS = 16
PAIR_HEADS = HEADS // 4
HEAD_DIM = LANES
QCOLS = HEADS * HEAD_DIM // 2
FF = 6656
FFH = FF // 2
FFQ = FF // 4
ROWS = 64
CHUNK = 32
PAIR = 2 * ROWS
SEQ = 8192
ROPE_THETA = 500000.0
ROPE_FACTOR = 8.0
LOW_FREQ = 1.0
HIGH_FREQ = 4.0
ORIG_CTX = 8192.0
NORM_EPS = 1e-5
NEG_BIG = -1e30
EXP_SCALE = HEAD_DIM ** -0.5 * math.log2(math.e)

KC = 512
NB = 2048
N1 = 6
K_SLOT = 4
N2 = 9
BLOCKS_N = HALF // NB
Q_TRIPS = MODEL // (2 * KC)
O_CHUNKS = HEADS * HEAD_DIM // KC
O_WIDE = O_CHUNKS - 1
O_SLOTS = BLOCKS_N * O_WIDE
D_CHUNKS = FF // KC
D_OWN = D_CHUNKS // 2
D_REST = D_CHUNKS - D_OWN
D_FIRST = D_OWN * BLOCKS_N
D_SLOTS = D_CHUNKS * BLOCKS_N
D_EXTRA = N1
G_SLOTS = MODEL // KC
G_TRIPS = G_SLOTS // 2
BC = 2 * KC
BP = HALF // BC
XP = 4
PIECES_PER_SLOT = FFQ // LANES
KV_PIECES = MODEL // KC
KV_UNROLL = 8
HOOK_B, HOOK_C = 0, 10
PRE = 3
QL = 512
SCORE_BUFS = (0, 2 * QL)
NEAR = 6
STEPS = 18
DELIVER = 4096
NEIGHBOURS = (('x', 1), ('x', 3), ('y', 1), ('y', 3))
GROUPS = range(len(NEIGHBOURS))
GROUP = PAIR // len(NEIGHBOURS)

MESH = pl.DeviceIdType.MESH
F32 = jnp.float32
BF16 = jnp.bfloat16
BLOCKS = (((0, 1), 0, 'yzx'), ((1, 1), 0, 'zxy'), ((0, 2), 1, 'xyz'))
OWN = (0, 0, 0)
SENDS = ((OWN, 0), (OWN, 1), (OWN, 2), ((1, 0, 0), 1), ((1, 0, 0), 2), ((0, 1, 0), 2), ((1, 1, 0), 2))
ROUNDS = ((0, 1, 2), (3, 4, 5), (6,))
STEPS_ALONG = (1, 2, 3)


def dot(a, b):
    return jnp.dot(a, b, preferred_element_type=F32)


def span(first, count=LANES):
    return pl.ds(pl.multiple_of(first, LANES), count)


def iota(rows, cols, dim):
    return lax.broadcasted_iota(jnp.int32, (rows, cols), dim)


def rope_tables(pos):
    lane = iota(SUBLANES, HEAD_DIM, 1)
    j = lax.rem(lane, HEAD_DIM // 2).astype(F32)
    inv_freq = jnp.exp(j * (-2.0 / HEAD_DIM * math.log(ROPE_THETA)))
    wavelen = (2.0 * math.pi) / inv_freq
    smooth = jnp.clip((ORIG_CTX / wavelen - LOW_FREQ) / (HIGH_FREQ - LOW_FREQ), 0.0, 1.0)
    freq = ((1.0 - smooth) * inv_freq / ROPE_FACTOR + smooth * inv_freq)[:1]
    angle = pos * freq
    sign = jnp.where(lane[:1] < HEAD_DIM // 2, -1.0, 1.0)
    return jnp.cos(angle), jnp.sin(angle) * sign


def rope(t, cos_t, sin_t):
    return t * cos_t + pltpu.roll(t, HEAD_DIM // 2, 1) * sin_t


def layer_kernel(x_hbm, pos_ref, ag_ref, wq, wk, wv, wo, wo_rows, mg_ref, wg, wu, wd,
                 z_hbm, k_out, v_out,
                 x128, bbuf, w1, w2, acc, gacc, qt, ml, mx, obuf, mbuf, mst, st, ss, kst, gains,
                 xl_sem, xs_sem, xr_sem, sts_sem, str_sem, kvw_sem, w1_sem, w2_sem, gs_sem, gr_sem, fs_sem, fr_sem,
                 os_sem, or_sem, sss_sem, ssr_sem, bs_sem, br_sem, ns_sem, nr_sem, ms_sem, mr_sem, nms_sem, nmr_sem,
                 zl_sem, zs_sem, zr_sem, ko_sem, spare_sem, free_sem):
    me = lax.axis_index('cp')
    core = lax.rem(me, 2)
    chip = lax.div(me, 2)
    coords = {'x': lax.rem(chip, SIDE), 'y': lax.rem(lax.div(chip, SIDE), SIDE), 'z': lax.div(chip, SIDE * SIDE)}
    cx, cy, cz = coords['x'], coords['y'], coords['z']
    other = 1 - core
    sib = me + other - core
    color = lax.rem(cx + cy + cz, 2)
    hidden = pl.multiple_of(color * FFH + core * FFQ, LANES)

    def peer(dim, k, to_core=core):
        c = dict(coords)
        c[dim] = lax.rem(c[dim] + k, SIDE)
        return ((c['z'] * SIDE + c['y']) * SIDE + c['x']) * 2 + to_core

    def remote(src, dst, s, r, dev):
        return pltpu.make_async_remote_copy(src, dst, s, r, device_id={'cp': dev}, device_id_type=MESH)

    def to_sib(src, dst, s, r):
        return remote(src, dst, s, r, sib)

    own_rows = pl.ds(pl.multiple_of(core * ROWS, ROWS), ROWS)
    sib_rows = pl.ds(pl.multiple_of(other * ROWS, ROWS), ROWS)
    pair_rows = pl.ds(0, PAIR)
    own_half = pl.multiple_of(core * HALF, HALF)
    sib_half = pl.multiple_of(other * HALF, HALF)

    def w_rows(first):
        return pl.ds(lax.div(first, KC // 2), 2)

    def kv_dst(c, i):
        return w1.at[lax.div(c, PIECES_PER_SLOT), pl.ds(2 * i, 2), :, :, span(lax.rem(c, PIECES_PER_SLOT) * LANES)]

    def kv_copy(c, i):
        return pltpu.make_async_copy((wk, wv)[i].at[w_rows(c * KC)], kv_dst(c, i), kvw_sem.at[i, c])

    def o_chunk(u):
        return lax.rem(u + 2 * core, O_CHUNKS)

    def o_spare(n, h):
        rows = pl.ds(o_chunk(O_WIDE) * KC + h * PAIR * 2, PAIR * 2)
        return pltpu.make_async_copy(wo_rows.at[rows, span(own_half + n * NB, NB)], bbuf.at[:, span((2 * n + h) * NB, NB)], spare_sem.at[n, h])

    def d_place(i):
        first = i < D_FIRST
        n = jnp.where(first, lax.rem(i, BLOCKS_N), lax.div(i - D_FIRST, D_REST))
        return n, jnp.where(first, lax.div(i, BLOCKS_N), D_OWN + lax.rem(i - D_FIRST, D_REST))

    def d_chunk(kk):
        mine = color * D_REST + jnp.where(core == 0, kk, D_OWN - 1 - kk)
        return jnp.where(kk < D_OWN, mine, jnp.where(kk == D_OWN, D_OWN, (other_color * D_REST) + kk - D_REST))

    other_color = 1 - color

    def w2_start(n):
        slot = lax.rem(n, N2)

        @pl.when(n < Q_TRIPS)
        def _():
            for h in range(2):
                src = wq.at[w_rows(n * (2 * KC) + h * KC), :, :, span(core * QCOLS, QCOLS)]
                pltpu.make_async_copy(src, w2.at[slot, :, :, :, pl.ds(h * QCOLS, QCOLS)], w2_sem.at[slot]).start()

        @pl.when((n >= Q_TRIPS) & (n < Q_TRIPS + O_SLOTS))
        def _():
            i = n - Q_TRIPS
            src = wo.at[w_rows(o_chunk(lax.rem(i, O_WIDE)) * KC), :, :, span(own_half + lax.div(i, O_WIDE) * NB, NB)]
            pltpu.make_async_copy(src, w2.at[slot], w2_sem.at[slot]).start()

        @pl.when((n >= Q_TRIPS + O_SLOTS) & (n < Q_TRIPS + O_SLOTS + D_SLOTS - D_EXTRA))
        def _():
            i = n - (Q_TRIPS + O_SLOTS)
            block, kk = d_place(jnp.where(i < N2, i, i + D_EXTRA))
            src = wd.at[w_rows(d_chunk(kk) * KC), :, :, span(own_half + block * NB, NB)]
            pltpu.make_async_copy(src, w2.at[slot], w2_sem.at[slot]).start()

    def w2_wait(n):
        slot = lax.rem(n, N2)
        pltpu.make_async_copy(wo.at[w_rows(0), :, :, span(0, NB)], w2.at[slot], w2_sem.at[slot]).wait()
        return slot

    def wide(slot):
        return w2[slot].reshape(KC, NB)

    def g_cols(t):
        return pl.multiple_of(jnp.where(t < BP, own_half, sib_half) + lax.rem(t, BP) * BC, BC)

    def w1_start(n):
        slot = lax.rem(n, N1)

        @pl.when(n < G_SLOTS)
        def _():
            for i, w in enumerate((wg, wu)):
                src = w.at[w_rows(g_cols(lax.div(n, 2)) + lax.rem(n, 2) * KC), :, :, span(hidden, FFQ)]
                pltpu.make_async_copy(src, w1.at[slot, pl.ds(2 * i, 2)], w1_sem.at[slot]).start()

        @pl.when(n >= G_SLOTS)
        def _():
            block, kk = d_place(n - G_SLOTS + N2)
            for h in range(2):
                src = wd.at[w_rows(d_chunk(kk) * KC), :, :, span(own_half + block * NB + h * BC, BC)]
                pltpu.make_async_copy(src, w1.at[slot, pl.ds(2 * h, 2), :, :, span(0, BC)], w1_sem.at[slot]).start()

    def w1_wait(n):
        slot = lax.rem(n, N1)
        pltpu.make_async_copy(wg.at[pl.ds(0, SIDE), :, :, span(0, FFQ)], w1.at[slot], w1_sem.at[slot]).wait()
        return slot

    def w1_wait_down(n):
        slot = lax.rem(n, N1)
        pltpu.make_async_copy(wd.at[pl.ds(0, SIDE), :, :, span(0, BC)], w1.at[slot, :, :, :, span(0, BC)], w1_sem.at[slot]).wait()
        return slot

    x_local = pltpu.make_async_copy(x_hbm, x128.at[own_rows, :], xl_sem)
    x_local.start()
    barrier = pltpu.get_barrier_semaphore()
    greeted = [sib] + [peer(dim, k) for dim in 'xyz' for k in STEPS_ALONG] + [peer(dim, k, other) for dim, k in NEIGHBOURS]
    for dev in greeted:
        pl.semaphore_signal(barrier, device_id={'cp': dev}, device_id_type=MESH)

    @pl.loop(0, KV_PIECES)
    def _(c):
        for i in range(2):
            kv_copy(c, i).start()

    def x_copy(i):
        cols = span(i * (MODEL // XP), MODEL // XP)
        return to_sib(x_hbm.at[:, cols], x128.at[own_rows, cols], xs_sem.at[i], xr_sem.at[i])

    eye = iota(ROWS, ROWS, 0) == iota(ROWS, ROWS, 1)
    pos_own = jnp.sum(jnp.where(eye, jnp.broadcast_to(pos_ref[...].astype(F32), (ROWS, ROWS)), 0.0), axis=1, keepdims=True)
    cos_own, sin_own = rope_tables(pos_own)
    gains[0] = ag_ref[...].astype(F32)
    gains[1] = mg_ref[...].astype(F32)

    x_local.wait()

    def square_sum(i, part):
        for u in range(SUBLANES):
            v = x128[own_rows, span(i * BC + u * LANES)].astype(F32)
            part = part + v * v
        return part

    part = lax.fori_loop(0, MODEL // BC, square_sum, jnp.zeros((ROWS, LANES), F32))
    inv_own = lax.rsqrt(jnp.sum(part, axis=1, keepdims=True) / MODEL + NORM_EPS)
    pl.semaphore_wait(barrier, len(greeted))
    for i in range(XP):
        x_copy(i).start()
    st[core] = jnp.where(iota(ROWS, LANES, 1) == 0, inv_own, pos_own)
    st_copy = to_sib(st.at[core], st.at[core], sts_sem, str_sem)
    st_copy.start()

    def normalize(rows, inv, lo, hi):
        @pl.loop(lo, hi)
        def _(i):
            for u in range(SUBLANES):
                tile = i * SUBLANES + u
                cols = span(tile * LANES)
                bbuf[rows, cols] = (x128[rows, cols].astype(F32) * inv * gains[0, pl.ds(tile, 1), :]).astype(BF16)

    normalize(own_rows, inv_own, 0, MODEL // BC)

    @pl.loop(0, N2)
    def _(n):
        w2_start(n)

    def kv_trip(i, total):
        places = [i * KV_UNROLL + u for u in range(KV_UNROLL)]
        for c in places:
            for j in range(2):
                kv_copy(c, j).wait()
        for c in places:
            w = jnp.concatenate([kv_dst(c, j)[...].reshape(KC, LANES) for j in range(2)], axis=1)
            total = total + dot(bbuf[own_rows, span(c * KC, KC)], w)
        return total

    kv_raw = lax.fori_loop(0, KV_PIECES // KV_UNROLL, kv_trip, jnp.zeros((ROWS, 2 * LANES), F32))
    r0 = (pl.multiple_of(core * CHUNK, CHUNK), pl.multiple_of(other * CHUNK, CHUNK))
    stores = []
    for i, (t, out) in enumerate(((rope(kv_raw[:, :LANES], cos_own, sin_own), k_out), (kv_raw[:, LANES:], v_out))):
        t = t.astype(BF16)
        w1[K_SLOT + i, 0, 0, pl.ds(r0[0], CHUNK), :LANES] = t[:CHUNK]
        w1[K_SLOT + i, 0, 0, pl.ds(r0[1], CHUNK), span(SIDE * LANES)] = t[CHUNK:]
        kst[i] = t
        stores.append(pltpu.make_async_copy(kst.at[i], out, ko_sem.at[i]))
        stores[i].start()

    def region(b, spec, dim=None, place=None, rows=0):
        slots, half, dims = BLOCKS[b]

        def at(d):
            first, count = (place, 1) if d == dim else (1, SIDE - 1) if spec[dims.index(d)] else (0, 1)
            return first, count

        first, count = at('z')
        lanes = pl.ds((half * SIDE + first) * LANES, count * LANES)
        rows = pl.ds(r0[half if rows == 0 else 1 - half], CHUNK)
        return w1.at[pl.ds(K_SLOT + slots[0], slots[1]), pl.ds(*at('y')), pl.ds(*at('x')), rows, lanes]

    def gather_copy(b, n, k):
        spec, along = SENDS[n]
        dim = BLOCKS[b][2][along]
        return remote(region(b, spec), region(b, spec, dim, SIDE - k), gs_sem.at[b, n, k - 1], gr_sem.at[b, n, k - 1], peer(dim, k))

    def forward(b, n, k, rows=0):
        spec, along = SENDS[n]
        part = region(b, spec, BLOCKS[b][2][along], SIDE - k, rows)
        return to_sib(part, part, fs_sem.at[b, n, k - 1], fr_sem.at[b, n, k - 1])

    def own_forward(b, rows=0):
        part = region(b, OWN, rows=rows)
        return to_sib(part, part, fs_sem.at[b, len(SENDS), 0], fr_sem.at[b, len(SENDS), 0])

    def each(sends, side, action):
        for n in sends:
            for b in range(len(BLOCKS)):
                for k in STEPS_ALONG:
                    if BLOCKS[b][1] == 1 and BLOCKS[b][2][SENDS[n][1]] == 'z':
                        pl.when(cz + k >= SIDE if side == 'send' else cz < k)(functools.partial(action, b, n, k))
                    else:
                        action(b, n, k)

    def send(b, n, k):
        gather_copy(b, n, k).start()

    def sent(b, n, k):
        gather_copy(b, n, k).wait_send()

    def receive(b, n, k):
        gather_copy(b, n, k).wait_recv()

    def pass_on(b, n, k):
        forward(b, n, k).start()

    def receive_pass_on(b, n, k):
        receive(b, n, k)
        pass_on(b, n, k)

    def passed(b, n, k):
        forward(b, n, k).wait_send()
        forward(b, n, k, 1).wait_recv()

    each(ROUNDS[0], 'send', send)
    for b in range(len(BLOCKS)):
        own_forward(b).start()

    def second_round():
        each(ROUNDS[0][:2], 'recv', receive)
        each(ROUNDS[1], 'send', send)
        each(ROUNDS[0][:2], 'recv', pass_on)
        each(ROUNDS[0][2:], 'recv', receive_pass_on)

    def third_round():
        each(ROUNDS[1][:1], 'recv', receive)
        each(ROUNDS[2], 'send', send)
        each(ROUNDS[1][:1], 'recv', pass_on)

    def own_plane_there():
        each(ROUNDS[1][1:], 'recv', receive_pass_on)
        for b in range(len(BLOCKS)):
            own_forward(b).wait_send()
            own_forward(b, 1).wait_recv()
        each(ROUNDS[0] + ROUNDS[1], 'recv', passed)

    def all_there():
        each(ROUNDS[2], 'recv', receive_pass_on)
        each(ROUNDS[2], 'recv', passed)

    st_copy.wait()
    inv_sib = st[other][:, :1]
    for i in range(XP):
        x_copy(i).wait()
        normalize(sib_rows, inv_sib, i * XP, (i + 1) * XP)

    acc[0] = jnp.zeros((PAIR, NB), F32)

    @pl.loop(0, Q_TRIPS)
    def _(i):
        pl.when(i == HOOK_B)(second_round)
        pl.when(i == HOOK_C)(third_round)
        w = wide(w2_wait(i))
        acc[0, :, :QCOLS] += (dot(bbuf[pair_rows, span(i * BC, KC)], w[:, :QCOLS])
                              + dot(bbuf[pair_rows, span(i * BC + KC, KC)], w[:, QCOLS:]))
        w2_start(i + N2)

    for n in range(BLOCKS_N):
        for h in range(2):
            o_spare(n, h).start()

    @pl.loop(0, K_SLOT)
    def _(n):
        w1_start(n)

    pos_all = jnp.concatenate([st[i][:, 1:2] for i in range(2)], axis=0)
    cos_t, sin_t = rope_tables(pos_all)
    EARLY = (slice(0, CHUNK), slice(ROWS, ROWS + CHUNK))
    LATE = (slice(ROWS + CHUNK, PAIR), slice(CHUNK, ROWS))
    for hp in range(PAIR_HEADS):
        q = [rope(acc[0, :, span(h * LANES)], cos_t, sin_t) for h in (2 * hp, 2 * hp + 1)]
        for half, rows in enumerate((EARLY, LATE)):
            qt[half, :, span(hp * LANES)] = jnp.concatenate([v[r] for v in q for r in rows], axis=0).T.astype(BF16)

    own_plane_there()
    ml[:, 0] = jnp.full((2, SUBLANES, QL), NEG_BIG, F32)
    ml[:, 1] = jnp.zeros((2, SUBLANES, QL), F32)
    acc[:2, :, :QL] = jnp.zeros((2, HEAD_DIM, QL), F32)
    row_of = iota(PAIR, LANES, 0)
    r64 = lax.rem(iota(PAIR, LANES, 1), ROWS)

    def row_positions(rows):
        src = jnp.where(r64 < CHUNK, r64 + rows[0].start, r64 + (rows[1].start - CHUNK))
        return jnp.sum(jnp.where(row_of == src, pos_all, 0.0), axis=0, keepdims=True).astype(jnp.int32)

    pos_e, pos_l = row_positions(EARLY), row_positions(LATE)

    def natural(late, c):
        return jnp.where(late, SEQ - ROWS * (c + 1), ROWS * c)

    def step(s):
        near = s < NEAR
        r = lax.div(s - NEAR, 2)
        late_q = jnp.where(near, s >= 2, r >= cz)
        late_k = jnp.where(near, lax.div(s, 2) == 1, late_q & (r < SIDE - 1))
        dz = jnp.where(near, 0, jnp.where(late_q, jnp.where(r < SIDE - 1, r - cz + 1, r - 2), SIDE - 1 - r))
        lanes = span((late_k.astype(jnp.int32) * SIDE + dz) * LANES)
        return late_q, late_k, dz, lax.rem(s, 2) * 2, lanes

    def product(s, buf):
        late_q, late_k, dz, dy, lanes = step(s)
        q = qt[late_q.astype(jnp.int32)]
        row_nat = natural(late_q, chip) + r64[:1]
        row_first = row_nat - jnp.where(late_q, pos_l, pos_e)
        plane = lax.rem(cz + dz, SIDE) * SIDE
        u = iota(ROWS, 1, 0)
        tops = [jnp.full((SUBLANES, LANES), NEG_BIG, F32)] * SIDE
        for part in range(2):
            keys = w1[K_SLOT, dy + part, :, :, lanes].reshape(SIDE * ROWS, LANES)
            row_y = (plane + lax.rem(cy + dy + part, SIDE)) * SIDE
            scores = dot(keys, q)
            for i in range(SIDE):
                key_nat = natural(late_k, row_y + lax.rem(cx + i, SIDE)) + u
                visible = (key_nat >= row_first) & (key_nat <= row_nat)
                rows = slice(i * ROWS, (i + 1) * ROWS)
                for l in range(SIDE):
                    tile = jnp.where(visible, scores[rows, l * LANES:(l + 1) * LANES], NEG_BIG)
                    gacc[rows, span(SCORE_BUFS[buf] + part * QL + l * LANES)] = tile
                    for r in range(0, ROWS, SUBLANES):
                        tops[l] = jnp.maximum(tops[l], tile[r:r + SUBLANES])
        mx[buf] = jnp.concatenate(tops, axis=1)

    def soften(s, buf):
        late_q, _, _, dy, lanes = step(s)
        qh = late_q.astype(jnp.int32)
        m_old = ml[qh, 0, :1]
        m_new = jnp.maximum(m_old, jnp.max(mx[buf], axis=0, keepdims=True))
        shift = m_new * EXP_SCALE
        p = jnp.concatenate([jnp.exp2(gacc[:, span(SCORE_BUFS[buf] + i * QL, QL)] * EXP_SCALE - shift) for i in range(2)], axis=0)
        alpha = jnp.exp2((m_old - m_new) * EXP_SCALE)
        ml[qh, 0, :1] = m_new
        ml[qh, 1, :1] = ml[qh, 1, :1] * alpha + jnp.sum(p, axis=0, keepdims=True)
        vals = w1[K_SLOT + 1, pl.ds(dy, 2), :, :, lanes].reshape(2 * SIDE * ROWS, LANES)
        pv = lax.dot_general(vals, p.astype(BF16), (((0,), (0,)), ((), ())), preferred_element_type=F32)
        acc[qh, :, :QL] = acc[qh, :, :QL] * alpha + pv

    product(0, 0)

    @pl.loop(0, STEPS // 2)
    def _(i):
        @pl.when(i == NEAR // 2)
        def _():
            all_there()
            product(NEAR, 0)

        product(2 * i + 1, 1)
        soften(2 * i, 0)
        product(jnp.where((i == NEAR // 2 - 1) | (i == STEPS // 2 - 1), 0, 2 * i + 2), 0)
        soften(2 * i + 1, 1)

    for hp in range(PAIR_HEADS):
        for half, rows in enumerate((EARLY, LATE)):
            o = (acc[half, :, span(hp * LANES)] / ml[half, 1, :1, span(hp * LANES)]).T.astype(BF16)
            for u in range(2):
                for i, r in enumerate(rows):
                    obuf[core, r, span((2 * hp + u) * LANES)] = o[ROWS * u + CHUNK * i:ROWS * u + CHUNK * (i + 1)]
    o_copy = to_sib(obuf.at[core], obuf.at[core], os_sem, or_sem)
    o_copy.start()
    each(range(len(SENDS)), 'send', sent)
    for n in range(K_SLOT, N1):
        w1_start(n)

    def o_part(n, own):
        group = core if own else other
        places = range(2) if own else range(2, O_WIDE)
        slots = [w2_wait(Q_TRIPS + O_WIDE * n + u) for u in places]

        def part(cols):
            terms = [dot(obuf[group, :, u % 2 * KC:(u % 2 + 1) * KC], w2[s, :, :, :, cols].reshape(KC, QL)) for u, s in zip(places, slots)]
            if not own:
                for h in range(2):
                    w = bbuf[:, span((2 * n + h) * NB + cols.start, QL)]
                    terms.append(dot(obuf[group, :, span(KC + h * PAIR * 2, PAIR * 2)], w))
            return sum(terms)

        return part

    def o_block(n, parts):
        total = jnp.zeros((PAIR, LANES), F32)
        for h in range(2):
            o_spare(n, h).wait()
        for b in range(0, NB, QL):
            out = sum(p(slice(b, b + QL)) for p in parts)
            cols = span(own_half + n * NB + b, QL)
            h = (x128[:, cols].astype(F32) + out).astype(BF16)
            x128[:, cols] = h
            hf = h.astype(F32)
            for u in range(0, QL, LANES):
                total = total + hf[:, u:u + LANES] * hf[:, u:u + LANES]
        ss[core] += total
        for u in range(O_WIDE):
            w2_start(Q_TRIPS + O_WIDE * n + u + N2)

    ss[core] = jnp.zeros((PAIR, LANES), F32)
    first = o_part(0, True)
    for b in range(0, NB, QL):
        acc[0, :, b:b + QL] = first(slice(b, b + QL))
    o_copy.wait()
    o_block(0, [lambda cols: acc[0, :, cols], o_part(0, False)])

    @pl.loop(1, BLOCKS_N)
    def _(n):
        o_block(n, [o_part(n, True), o_part(n, False)])

    for dim, k in NEIGHBOURS:
        for c in range(2):
            pl.semaphore_signal(free_sem, device_id={'cp': peer(dim, SIDE - k, c)}, device_id_type=MESH)
    ss_copy = to_sib(ss.at[core], ss.at[core], sss_sem, ssr_sem)
    ss_copy.start()
    gacc[...] = jnp.zeros_like(gacc)
    ss_copy.wait()
    inv_h = lax.rsqrt(jnp.sum(ss[0] + ss[1], axis=1, keepdims=True) / MODEL + NORM_EPS)

    def b_copy(i, half=own_half):
        part = bbuf.at[pair_rows, span(half + i * BC, BC)]
        return to_sib(part, part, bs_sem.at[i], br_sem.at[i])

    def n_copy(cross, i, g):
        dim, k = NEIGHBOURS[g]
        cols = span(own_half + i * BC, BC)
        return remote(bbuf.at[pl.ds(g * GROUP, GROUP), cols], bbuf.at[pl.ds(PAIR + g * GROUP, GROUP), cols],
                      ns_sem.at[cross, i, g], nr_sem.at[cross, i, g], peer(dim, k, other if cross else core))

    def n_arrival(cross, i, g):
        dim, k = NEIGHBOURS[g]
        dst = bbuf.at[pl.ds(PAIR + g * GROUP, GROUP), span((sib_half if cross else own_half) + i * BC, BC)]
        return remote(dst, dst, ns_sem.at[cross, i, g], nr_sem.at[cross, i, g], peer(dim, SIDE - k, other if cross else core))

    pl.semaphore_wait(free_sem, 2 * len(NEIGHBOURS))

    @pl.loop(0, BP)
    def _(i):
        for j in range(BC // LANES):
            tile = core * (HALF // LANES) + i * (BC // LANES) + j
            cols = span(tile * LANES)
            bbuf[pair_rows, cols] = (x128[:, cols].astype(F32) * inv_h * gains[1, pl.ds(tile, 1), :]).astype(BF16)
        for g in GROUPS:
            n_copy(0, i, g).start()
        b_copy(i).start()

    @pl.loop(0, BP)
    def _(i):
        for g in GROUPS:
            n_copy(1, i, g).start()

    def gate_up(rows, t, slots):
        parts = [(bbuf[rows, span(g_cols(t) + u * KC, KC)], s) for u, s in enumerate(slots)]

        def block(i, cols):
            return [w1[s, 2 * i:2 * i + 2, :, :, cols].reshape(KC, cols.stop - cols.start) for _, s in parts]

        def product_of(weights):
            return sum(dot(a, w) for (a, _), w in zip(parts, weights))

        for i in range(2):
            for b in range(0, FFQ - LANES, QL):
                gacc[rows, i * FFQ + b:i * FFQ + b + QL] += product_of(block(i, slice(b, b + QL)))
        last = slice(FFQ - LANES, FFQ)
        pair = product_of([jnp.concatenate(w, axis=1) for w in zip(block(0, last), block(1, last))])
        gacc[rows, last] += pair[:, :LANES]
        gacc[rows, 2 * FFQ - LANES:] += pair[:, LANES:]

    def refill(t):
        for u in range(2):
            w1_start(2 * t + u + N1)

    @pl.loop(0, PRE)
    def _(t):
        gate_up(slice(0, PAIR), t, [w1_wait(2 * t + u) for u in range(2)])

    @pl.loop(0, PRE)
    def _(t):
        for g in GROUPS:
            n_arrival(0, t, g).wait_recv()
        gate_up(slice(PAIR, 2 * PAIR), t, [2 * t + u for u in range(2)])
        refill(t)

    @pl.loop(PRE, G_TRIPS)
    def _(t):
        @pl.when(t < BP)
        def _():
            for g in GROUPS:
                n_arrival(0, t, g).wait_recv()

        @pl.when(t >= BP)
        def _():
            b_copy(t - BP, sib_half).wait_recv()
            for g in GROUPS:
                n_arrival(1, t - BP, g).wait_recv()

        gate_up(slice(0, 2 * PAIR), t, [w1_wait(2 * t + u) for u in range(2)])
        refill(t)

    def gated(rows, j):
        g = gacc[rows, span(j * LANES)]
        return (g * (1.0 / (1.0 + jnp.exp(-g))) * gacc[rows, span(FFQ + j * LANES)]).astype(BF16)

    @pl.loop(0, FFQ // LANES)
    def _(j):
        mst[:, span(j * LANES)] = gated(pl.ds(PAIR, PAIR), j)

    def nm_copy(cross, g):
        dim, k = NEIGHBOURS[g]
        return remote(mst.at[pl.ds(g * GROUP, GROUP), :], mbuf.at[pl.ds(g * GROUP, GROUP), span(hidden, FFQ)],
                      nms_sem.at[cross, g], nmr_sem.at[cross, g], peer(dim, SIDE - k, other if cross else core))

    def nm_arrival(cross, g):
        dim, k = NEIGHBOURS[g]
        dst = mbuf.at[pl.ds(g * GROUP, GROUP), span(other_color * FFH + (other if cross else core) * FFQ, FFQ)]
        return remote(dst, dst, nms_sem.at[cross, g], nmr_sem.at[cross, g], peer(dim, k, other if cross else core))

    for cross in range(2):
        for g in GROUPS:
            nm_copy(cross, g).start()

    @pl.loop(0, FFQ // LANES)
    def _(j):
        mbuf[:, span(hidden + j * LANES)] = gated(pair_rows, j)

    def m_copy(of_core):
        part = mbuf.at[:, span(color * FFH + of_core * FFQ, FFQ)]
        return to_sib(part, part, ms_sem, mr_sem)

    m_copy(core).start()

    acc[...] = jnp.zeros_like(acc)

    @pl.loop(0, BP)
    def _(i):
        b_copy(i).wait_send()
        for cross in range(2):
            for g in GROUPS:
                n_copy(cross, i, g).wait_send()

    def z_cols(n, half=own_half):
        return span(half + n * NB, NB)

    def z_local(n):
        return pltpu.make_async_copy(bbuf.at[own_rows, z_cols(n)], z_hbm.at[:, z_cols(n)], zl_sem.at[n])

    def z_remote(n, half=own_half):
        return to_sib(bbuf.at[sib_rows, z_cols(n)], z_hbm.at[:, z_cols(n, half)], zs_sem.at[n], zr_sem.at[n])

    def down(i, weight):
        n, kk = d_place(i)
        a = mbuf[:, span(d_chunk(kk) * KC, KC)]
        acc[n] += dot(a, weight)

    @pl.loop(0, N2)
    def _(i):
        @pl.when(i == 2 * BLOCKS_N)
        def _():
            m_copy(core).wait_send()
            m_copy(other).wait_recv()

        down(i, wide(w2_wait(Q_TRIPS + O_SLOTS + i)))
        w2_start(Q_TRIPS + O_SLOTS + i + N2)

    @pl.loop(0, D_EXTRA)
    def _(i):
        slot = w1_wait_down(G_SLOTS + i)
        down(i + N2, jnp.concatenate([w1[slot, 2 * h:2 * h + 2, :, :, :BC].reshape(KC, BC) for h in range(2)], axis=1))

    @pl.loop(N2, D_SLOTS - D_EXTRA)
    def _(j):
        i = j + D_EXTRA

        @pl.when(i == D_FIRST)
        def _():
            for cross in range(2):
                for g in GROUPS:
                    nm_arrival(cross, g).wait_recv()

        down(i, wide(w2_wait(Q_TRIPS + O_SLOTS + j)))
        w2_start(Q_TRIPS + O_SLOTS + j + N2)
        n, kk = d_place(i)

        @pl.when(kk == D_CHUNKS - 1)
        def _():
            @pl.loop(0, NB // QL)
            def _(b):
                cols = span(own_half + n * NB + b * QL, QL)
                bbuf[pair_rows, cols] = (x128[:, cols].astype(F32) + acc[n, :, span(b * QL, QL)]).astype(BF16)

            z_local(n).start()
            z_remote(n).start()

    for n in range(BLOCKS_N):
        z_local(n).wait()
        z_remote(n).wait_send()
        z_remote(n, sib_half).wait_recv()
    for cross in range(2):
        for g in GROUPS:
            nm_copy(cross, g).wait_send()
    for s in stores:
        s.wait()


def deliver_kernel(z_in, k_in, v_in, z_out, k_out, v_out, zb, kb, in_sem, out_sem):
    moves = [(k_in, kb.at[0], k_out), (v_in, kb.at[1], v_out)]
    for first in range(0, MODEL, DELIVER):
        cols = span(first, DELIVER)
        moves.append((z_in.at[:, cols], zb.at[:, cols], z_out.at[:, cols]))
    moves = [(pltpu.make_async_copy(src, mid, in_sem.at[i]), pltpu.make_async_copy(mid, dst, out_sem.at[i])) for i, (src, mid, dst) in enumerate(moves)]
    for come, _ in moves:
        come.start()
    for come, go in moves:
        come.wait()
        go.start()
    for _, go in moves:
        go.wait()


def solution(mesh):
    def device_fn(x_loc, seg_loc, pos_loc, attn_gain, w_q, w_k, w_v, w_o, mlp_gain, w_gate, w_up, w_down):
        any_space = pl.BlockSpec(memory_space=pl.ANY)
        vmem = pl.BlockSpec(memory_space=pltpu.VMEM)

        def blocks(w):
            return w.reshape(-1, SIDE, ROWS, w.shape[1])

        def gain(g):
            return g.reshape(-1, LANES)

        z_shape, k_shape = (jax.ShapeDtypeStruct((ROWS, n), BF16) for n in (MODEL, HEAD_DIM))
        outs = (z_shape, k_shape, k_shape)
        f32_buffers = ((BLOCKS_N, PAIR, NB), (2 * PAIR, 2 * FFQ))
        stats = ((2, 2, SUBLANES, QL), (2, SUBLANES, QL))
        sems = {
            'xl': (), 'xs': (XP,), 'xr': (XP,), 'sts': (), 'str': (), 'kvw': (2, KV_PIECES), 'w1': (N1,), 'w2': (N2,),
            'gs': (len(BLOCKS), len(SENDS), len(STEPS_ALONG)), 'gr': (len(BLOCKS), len(SENDS), len(STEPS_ALONG)),
            'fs': (len(BLOCKS), len(SENDS) + 1, len(STEPS_ALONG)), 'fr': (len(BLOCKS), len(SENDS) + 1, len(STEPS_ALONG)),
            'os': (), 'or': (), 'sss': (), 'ssr': (), 'bs': (BP,), 'br': (BP,), 'ns': (2, BP, len(GROUPS)), 'nr': (2, BP, len(GROUPS)),
            'ms': (), 'mr': (), 'nms': (2, len(GROUPS)), 'nmr': (2, len(GROUPS)), 'zl': (BLOCKS_N,), 'zs': (BLOCKS_N,), 'zr': (BLOCKS_N,), 'ko': (2,), 'spare': (BLOCKS_N, 2),
        }

        def dma(shape):
            return pltpu.SemaphoreType.DMA(shape) if shape else pltpu.SemaphoreType.DMA

        results = pl.pallas_call(
            layer_kernel,
            out_shape=outs,
            in_specs=[any_space, vmem, vmem, any_space, any_space, any_space, any_space, any_space, vmem, any_space, any_space, any_space],
            out_specs=(any_space,) * len(outs),
            scratch_shapes=[
                pltpu.VMEM((PAIR, MODEL), BF16),
                pltpu.VMEM((2 * PAIR, MODEL), BF16),
                pltpu.VMEM((N1, SIDE, SIDE, ROWS, FFQ), BF16),
                pltpu.VMEM((N2, 2, SIDE, ROWS, NB), BF16),
                *(pltpu.VMEM(s, F32) for s in f32_buffers),
                pltpu.VMEM((2, HEAD_DIM, QL), BF16),
                *(pltpu.VMEM(s, F32) for s in stats),
                pltpu.VMEM((2, PAIR, QCOLS), BF16),
                pltpu.VMEM((PAIR, FF), BF16),
                pltpu.VMEM((PAIR, FFQ), BF16),
                pltpu.VMEM((2, ROWS, LANES), F32),
                pltpu.VMEM((2, PAIR, LANES), F32),
                pltpu.VMEM((2, ROWS, LANES), BF16),
                pltpu.VMEM((2, LANES, LANES), F32),
                *(dma(s) for s in sems.values()),
                pltpu.SemaphoreType.REGULAR,
            ],
            compiler_params=pltpu.CompilerParams(collective_id=0, has_side_effects=True, vmem_limit_bytes=67043328),
            name='layer',
        )(x_loc[0], pos_loc.reshape(1, ROWS), gain(attn_gain), blocks(w_q), blocks(w_k), blocks(w_v), blocks(w_o), w_o, gain(mlp_gain),
          blocks(w_gate), blocks(w_up), blocks(w_down))
        moves = MODEL // DELIVER + 2
        z_rows, k_rows, v_rows = pl.pallas_call(
            deliver_kernel,
            out_shape=outs,
            in_specs=[any_space] * len(outs),
            out_specs=(any_space,) * len(outs),
            scratch_shapes=[pltpu.VMEM((ROWS, MODEL), BF16), pltpu.VMEM((2, ROWS, HEAD_DIM), BF16), dma((moves,)), dma((moves,))],
            compiler_params=pltpu.CompilerParams(vmem_limit_bytes=62914560),
            name='finish',
        )(*results)
        return z_rows[None], k_rows[:, None, :], v_rows[:, None, :]

    seq_spec = P(('dp', 'cp'))
    rows_spec, cache_spec = P('dp', 'cp', None), P(('dp', 'cp'), None, None)
    return jax.shard_map(device_fn, mesh=mesh, in_specs=(rows_spec, seq_spec, seq_spec) + (P(),) * 9, out_specs=(rows_spec, cache_spec, cache_spec), check_vma=False)
```

```python
import functools
import math

import jax
import jax.numpy as jnp
from jax import lax
from jax.experimental import pallas as pl
from jax.experimental.pallas import tpu as pltpu
from jax.sharding import PartitionSpec as P

LANES = 128
SUBLANES = 8
SIDE = 4
MODEL = 16384
HALF = MODEL // 2
QUARTER = MODEL // 4
HEADS = 16
PAIR_HEADS = HEADS // 4
HEAD_DIM = LANES
QCOLS = HEADS * HEAD_DIM // 2
FF = 6656
FFH = FF // 2
FFQ = FF // 4
ROWS = 64
CHUNK = 32
PAIR = 2 * ROWS
SEQ = 8192
ROPE_THETA = 500000.0
ROPE_FACTOR = 8.0
LOW_FREQ = 1.0
HIGH_FREQ = 4.0
ORIG_CTX = 8192.0
NORM_EPS = 1e-5
NEG_BIG = -1e30
EXP_SCALE = HEAD_DIM ** -0.5 * math.log2(math.e)

KC = 512
NB = 2048
N1 = 6
K_SLOT = 4
N2 = 9
BLOCKS_N = HALF // NB
Q_TRIPS = MODEL // (2 * KC)
O_CHUNKS = HEADS * HEAD_DIM // KC
O_WIDE = O_CHUNKS - 1
O_SLOTS = BLOCKS_N * O_WIDE
D_CHUNKS = FF // KC
D_OWN = D_CHUNKS // 2
D_REST = D_CHUNKS - D_OWN
D_BLOCKS = QUARTER // NB
D_FIRST = D_OWN * D_BLOCKS
D_SLOTS = D_CHUNKS * D_BLOCKS
D_WIDE = tuple(range(8)) + (12,) + tuple(range(15, 23))
D_NARROW = tuple(range(8, 12)) + (13, 14, 23, 24, 25)
G_SLOTS = MODEL // KC
G_TRIPS = G_SLOTS // 2
BC = 2 * KC
BP = HALF // BC
XP = 4
PIECES_PER_SLOT = FFQ // LANES
KV_PIECES = MODEL // KC
KV_UNROLL = 8
HOOK_B, HOOK_C = 0, 12
PRE = 2
QL = 512
SCORE_BUFS = (0, 2 * QL)
NEAR = 6
STEPS = 18
DELIVER = 4096
NEIGHBOURS = (('x', 1), ('x', 3), ('y', 1), ('y', 3))
GROUPS = range(len(NEIGHBOURS))
GROUP = PAIR // len(NEIGHBOURS)

MESH = pl.DeviceIdType.MESH
F32 = jnp.float32
BF16 = jnp.bfloat16
BLOCKS = (((0, 1), 0, 'yzx'), ((1, 1), 0, 'zxy'), ((0, 2), 1, 'xyz'))
OWN = (0, 0, 0)
SENDS = ((OWN, 0), (OWN, 1), (OWN, 2), ((1, 0, 0), 1), ((1, 0, 0), 2), ((0, 1, 0), 2), ((1, 1, 0), 2))
ROUNDS = ((0, 1, 2), (3, 4, 5), (6,))
STEPS_ALONG = (1, 2, 3)


def dot(a, b):
    return jnp.dot(a, b, preferred_element_type=F32)


def span(first, count=LANES):
    return pl.ds(pl.multiple_of(first, LANES), count)


def iota(rows, cols, dim):
    return lax.broadcasted_iota(jnp.int32, (rows, cols), dim)


def rope_tables(pos):
    lane = iota(SUBLANES, HEAD_DIM, 1)
    j = lax.rem(lane, HEAD_DIM // 2).astype(F32)
    inv_freq = jnp.exp(j * (-2.0 / HEAD_DIM * math.log(ROPE_THETA)))
    wavelen = (2.0 * math.pi) / inv_freq
    smooth = jnp.clip((ORIG_CTX / wavelen - LOW_FREQ) / (HIGH_FREQ - LOW_FREQ), 0.0, 1.0)
    freq = ((1.0 - smooth) * inv_freq / ROPE_FACTOR + smooth * inv_freq)[:1]
    angle = pos * freq
    sign = jnp.where(lane[:1] < HEAD_DIM // 2, -1.0, 1.0)
    return jnp.cos(angle), jnp.sin(angle) * sign


def rope(t, cos_t, sin_t):
    return t * cos_t + pltpu.roll(t, HEAD_DIM // 2, 1) * sin_t


def layer_kernel(x_hbm, pos_ref, ag_ref, wq, wk, wv, wo, wo_rows, mg_ref, wg, wu, wd,
                 z_hbm, k_out, v_out,
                 x128, bbuf, w1, w2, acc, gacc, qt, ml, mx, obuf, mbuf, st, ss, kst, gains,
                 xl_sem, xs_sem, xr_sem, sts_sem, str_sem, kvw_sem, w1_sem, w2_sem, gs_sem, gr_sem, fs_sem, fr_sem,
                 os_sem, or_sem, sss_sem, ssr_sem, bs_sem, br_sem, ns_sem, nr_sem, ms_sem, mr_sem, nms_sem, nmr_sem, fms_sem, fmr_sem, hs_sem, hr_sem,
                 za_sem, zb_sem, zl_sem, zs_sem, zr_sem, ko_sem, spare_sem, free_sem):
    me = lax.axis_index('cp')
    core = lax.rem(me, 2)
    chip = lax.div(me, 2)
    coords = {'x': lax.rem(chip, SIDE), 'y': lax.rem(lax.div(chip, SIDE), SIDE), 'z': lax.div(chip, SIDE * SIDE)}
    cx, cy, cz = coords['x'], coords['y'], coords['z']
    other = 1 - core
    sib = me + other - core
    color = lax.rem(cx + cy + cz, 2)
    hidden = pl.multiple_of(color * FFH + core * FFQ, LANES)

    def peer(dim, k, to_core=core):
        c = dict(coords)
        c[dim] = lax.rem(c[dim] + k, SIDE)
        return ((c['z'] * SIDE + c['y']) * SIDE + c['x']) * 2 + to_core

    def remote(src, dst, s, r, dev):
        return pltpu.make_async_remote_copy(src, dst, s, r, device_id={'cp': dev}, device_id_type=MESH)

    def to_sib(src, dst, s, r):
        return remote(src, dst, s, r, sib)

    own_rows = pl.ds(pl.multiple_of(core * ROWS, ROWS), ROWS)
    sib_rows = pl.ds(pl.multiple_of(other * ROWS, ROWS), ROWS)
    pair_rows = pl.ds(0, PAIR)

    def col_of(c, v):
        return lax.div(v, QUARTER) * HALF + c * QUARTER + lax.rem(v, QUARTER)

    def own_col(v):
        return col_of(core, v)

    def sib_col(v):
        return col_of(other, v)

    def w_rows(first):
        return pl.ds(lax.div(first, KC // 2), 2)

    def kv_dst(c, i):
        return w1.at[lax.div(c, PIECES_PER_SLOT), pl.ds(2 * i, 2), :, :, span(lax.rem(c, PIECES_PER_SLOT) * LANES)]

    def kv_copy(c, i):
        return pltpu.make_async_copy((wk, wv)[i].at[w_rows(c * KC)], kv_dst(c, i), kvw_sem.at[i, c])

    def o_chunk(u):
        return lax.rem(u + 2 * core, O_CHUNKS)

    def o_spare(n, h):
        rows = pl.ds(o_chunk(O_WIDE) * KC + h * PAIR * 2, PAIR * 2)
        return pltpu.make_async_copy(wo_rows.at[rows, span(own_col(n * NB), NB)], bbuf.at[:, span((2 * n + h) * NB, NB)], spare_sem.at[n, h])

    def d_place(i):
        first = i < D_FIRST
        n = jnp.where(first, lax.rem(i, D_BLOCKS), lax.div(i - D_FIRST, D_REST))
        return n, jnp.where(first, lax.div(i, D_BLOCKS), D_OWN + lax.rem(i - D_FIRST, D_REST))

    def d_chunk(kk):
        mine = color * D_REST + jnp.where(core == 0, kk, D_OWN - 1 - kk)
        return jnp.where(kk < D_OWN, mine, jnp.where(kk == D_OWN, D_OWN, (other_color * D_REST) + kk - D_REST))

    def d_source(i, first, count):
        n, kk = d_place(i)
        return wd.at[w_rows(d_chunk(kk) * KC), :, :, span(color * HALF + core * QUARTER + n * NB + first, count)]

    other_color = 1 - color

    def w2_start(n):
        slot = lax.rem(n, N2)

        @pl.when(n < Q_TRIPS)
        def _():
            for h in range(2):
                src = wq.at[w_rows(n * (2 * KC) + h * KC), :, :, span(core * QCOLS, QCOLS)]
                pltpu.make_async_copy(src, w2.at[slot, :, :, :, pl.ds(h * QCOLS, QCOLS)], w2_sem.at[slot]).start()

        @pl.when((n >= Q_TRIPS) & (n < Q_TRIPS + O_SLOTS))
        def _():
            i = n - Q_TRIPS
            src = wo.at[w_rows(o_chunk(lax.rem(i, O_WIDE)) * KC), :, :, span(own_col(lax.div(i, O_WIDE) * NB), NB)]
            pltpu.make_async_copy(src, w2.at[slot], w2_sem.at[slot]).start()

        @pl.when((n >= Q_TRIPS + O_SLOTS) & (n < Q_TRIPS + O_SLOTS + len(D_WIDE)))
        def _():
            j = n - (Q_TRIPS + O_SLOTS)
            i = jnp.where(j < D_WIDE[N2 - 2] + 1, j, jnp.where(j == N2 - 1, D_WIDE[N2 - 1], j + (D_WIDE[N2] - N2)))
            pltpu.make_async_copy(d_source(i, 0, NB), w2.at[slot], w2_sem.at[slot]).start()

    def w2_wait(n):
        slot = lax.rem(n, N2)
        pltpu.make_async_copy(wo.at[w_rows(0), :, :, span(0, NB)], w2.at[slot], w2_sem.at[slot]).wait()
        return slot

    def wide(slot):
        return w2[slot].reshape(KC, NB)

    def g_cols(t):
        return pl.multiple_of(col_of(jnp.where(t < BP, core, other), lax.rem(t, BP) * BC), BC)

    def w1_start(n):
        slot = lax.rem(n, N1)

        @pl.when(n < G_SLOTS)
        def _():
            for i, w in enumerate((wg, wu)):
                src = w.at[w_rows(g_cols(lax.div(n, 2)) + lax.rem(n, 2) * KC), :, :, span(hidden, FFQ)]
                pltpu.make_async_copy(src, w1.at[slot, pl.ds(2 * i, 2)], w1_sem.at[slot]).start()

        @pl.when(n >= G_SLOTS)
        def _():
            u = n - G_SLOTS
            i = jnp.where(u < SIDE, D_NARROW[0] + u, jnp.where(u < N1, D_NARROW[SIDE] - SIDE + u, D_NARROW[N1] - N1 + u))
            for h in range(2):
                pltpu.make_async_copy(d_source(i, h * BC, BC), w1.at[slot, pl.ds(2 * h, 2), :, :, span(0, BC)], w1_sem.at[slot]).start()

    def w1_wait(n):
        slot = lax.rem(n, N1)
        pltpu.make_async_copy(wg.at[pl.ds(0, SIDE), :, :, span(0, FFQ)], w1.at[slot], w1_sem.at[slot]).wait()
        return slot

    def w1_wait_down(n):
        slot = lax.rem(n, N1)
        pltpu.make_async_copy(wd.at[pl.ds(0, SIDE), :, :, span(0, BC)], w1.at[slot, :, :, :, span(0, BC)], w1_sem.at[slot]).wait()
        return slot

    x_local = pltpu.make_async_copy(x_hbm, x128.at[own_rows, :], xl_sem)
    x_local.start()
    barrier = pltpu.get_barrier_semaphore()
    greeted = [sib] + [peer(dim, k) for dim in 'xyz' for k in STEPS_ALONG] + [peer(dim, k, other) for dim, k in NEIGHBOURS]
    for dev in greeted:
        pl.semaphore_signal(barrier, device_id={'cp': dev}, device_id_type=MESH)

    @pl.loop(0, KV_PIECES)
    def _(c):
        for i in range(2):
            kv_copy(c, i).start()

    def x_copy(i):
        cols = span(i * (MODEL // XP), MODEL // XP)
        return to_sib(x_hbm.at[:, cols], x128.at[own_rows, cols], xs_sem.at[i], xr_sem.at[i])

    eye = iota(ROWS, ROWS, 0) == iota(ROWS, ROWS, 1)
    pos_own = jnp.sum(jnp.where(eye, jnp.broadcast_to(pos_ref[...].astype(F32), (ROWS, ROWS)), 0.0), axis=1, keepdims=True)
    cos_own, sin_own = rope_tables(pos_own)
    gains[0] = ag_ref[...].astype(F32)
    gains[1] = mg_ref[...].astype(F32)

    x_local.wait()

    def square_sum(i, part):
        for u in range(SUBLANES):
            v = x128[own_rows, span(i * BC + u * LANES)].astype(F32)
            part = part + v * v
        return part

    part = lax.fori_loop(0, MODEL // BC, square_sum, jnp.zeros((ROWS, LANES), F32))
    inv_own = lax.rsqrt(jnp.sum(part, axis=1, keepdims=True) / MODEL + NORM_EPS)
    pl.semaphore_wait(barrier, len(greeted))
    for i in range(XP):
        x_copy(i).start()
    st[core] = jnp.where(iota(ROWS, LANES, 1) == 0, inv_own, pos_own)
    st_copy = to_sib(st.at[core], st.at[core], sts_sem, str_sem)
    st_copy.start()

    def normalize(rows, inv, lo, hi):
        @pl.loop(lo, hi)
        def _(i):
            for u in range(SUBLANES):
                tile = i * SUBLANES + u
                cols = span(tile * LANES)
                bbuf[rows, cols] = (x128[rows, cols].astype(F32) * inv * gains[0, pl.ds(tile, 1), :]).astype(BF16)

    normalize(own_rows, inv_own, 0, MODEL // BC)

    @pl.loop(0, N2)
    def _(n):
        w2_start(n)

    def kv_trip(i, total):
        places = [i * KV_UNROLL + u for u in range(KV_UNROLL)]
        for c in places:
            for j in range(2):
                kv_copy(c, j).wait()
        for c in places:
            w = jnp.concatenate([kv_dst(c, j)[...].reshape(KC, LANES) for j in range(2)], axis=1)
            total = total + dot(bbuf[own_rows, span(c * KC, KC)], w)
        return total

    kv_raw = lax.fori_loop(0, KV_PIECES // KV_UNROLL, kv_trip, jnp.zeros((ROWS, 2 * LANES), F32))
    r0 = (pl.multiple_of(core * CHUNK, CHUNK), pl.multiple_of(other * CHUNK, CHUNK))
    stores = []
    for i, (t, out) in enumerate(((rope(kv_raw[:, :LANES], cos_own, sin_own), k_out), (kv_raw[:, LANES:], v_out))):
        t = t.astype(BF16)
        w1[K_SLOT + i, 0, 0, pl.ds(r0[0], CHUNK), :LANES] = t[:CHUNK]
        w1[K_SLOT + i, 0, 0, pl.ds(r0[1], CHUNK), span(SIDE * LANES)] = t[CHUNK:]
        kst[i] = t
        stores.append(pltpu.make_async_copy(kst.at[i], out, ko_sem.at[i]))
        stores[i].start()

    def region(b, spec, dim=None, place=None, rows=0):
        slots, half, dims = BLOCKS[b]

        def at(d):
            first, count = (place, 1) if d == dim else (1, SIDE - 1) if spec[dims.index(d)] else (0, 1)
            return first, count

        first, count = at('z')
        lanes = pl.ds((half * SIDE + first) * LANES, count * LANES)
        rows = pl.ds(r0[half if rows == 0 else 1 - half], CHUNK)
        return w1.at[pl.ds(K_SLOT + slots[0], slots[1]), pl.ds(*at('y')), pl.ds(*at('x')), rows, lanes]

    def gather_copy(b, n, k):
        spec, along = SENDS[n]
        dim = BLOCKS[b][2][along]
        return remote(region(b, spec), region(b, spec, dim, SIDE - k), gs_sem.at[b, n, k - 1], gr_sem.at[b, n, k - 1], peer(dim, k))

    def forward(b, n, k, rows=0):
        spec, along = SENDS[n]
        part = region(b, spec, BLOCKS[b][2][along], SIDE - k, rows)
        return to_sib(part, part, fs_sem.at[b, n, k - 1], fr_sem.at[b, n, k - 1])

    def own_forward(b, rows=0):
        part = region(b, OWN, rows=rows)
        return to_sib(part, part, fs_sem.at[b, len(SENDS), 0], fr_sem.at[b, len(SENDS), 0])

    def each(sends, side, action):
        for n in sends:
            for b in range(len(BLOCKS)):
                for k in STEPS_ALONG:
                    if BLOCKS[b][1] == 1 and BLOCKS[b][2][SENDS[n][1]] == 'z':
                        pl.when(cz + k >= SIDE if side == 'send' else cz < k)(functools.partial(action, b, n, k))
                    else:
                        action(b, n, k)

    def send(b, n, k):
        gather_copy(b, n, k).start()

    def sent(b, n, k):
        gather_copy(b, n, k).wait_send()

    def receive(b, n, k):
        gather_copy(b, n, k).wait_recv()

    def pass_on(b, n, k):
        forward(b, n, k).start()

    def receive_pass_on(b, n, k):
        receive(b, n, k)
        pass_on(b, n, k)

    def passed(b, n, k):
        forward(b, n, k).wait_send()
        forward(b, n, k, 1).wait_recv()

    each(ROUNDS[0], 'send', send)
    for b in range(len(BLOCKS)):
        own_forward(b).start()

    def second_round():
        each(ROUNDS[0][:2], 'recv', receive)
        each(ROUNDS[1], 'send', send)
        each(ROUNDS[0][:2], 'recv', pass_on)
        each(ROUNDS[0][2:], 'recv', receive_pass_on)

    def third_round():
        each(ROUNDS[1][:1], 'recv', receive)
        each(ROUNDS[2], 'send', send)
        each(ROUNDS[1][:1], 'recv', pass_on)

    def own_plane_there():
        each(ROUNDS[1][1:], 'recv', receive_pass_on)
        for b in range(len(BLOCKS)):
            own_forward(b).wait_send()
            own_forward(b, 1).wait_recv()
        each(ROUNDS[0] + ROUNDS[1], 'recv', passed)

    def all_there():
        each(ROUNDS[2], 'recv', receive_pass_on)
        each(ROUNDS[2], 'recv', passed)

    st_copy.wait()
    inv_sib = st[other][:, :1]
    for i in range(XP):
        x_copy(i).wait()
        normalize(sib_rows, inv_sib, i * XP, (i + 1) * XP)

    acc[0] = jnp.zeros((PAIR, NB), F32)

    @pl.loop(0, Q_TRIPS)
    def _(i):
        pl.when(i == HOOK_B)(second_round)
        pl.when(i == HOOK_C)(third_round)
        w = wide(w2_wait(i))
        acc[0, :, :QCOLS] += (dot(bbuf[pair_rows, span(i * BC, KC)], w[:, :QCOLS])
                              + dot(bbuf[pair_rows, span(i * BC + KC, KC)], w[:, QCOLS:]))
        w2_start(i + N2)

    for n in range(BLOCKS_N):
        for h in range(2):
            o_spare(n, h).start()

    @pl.loop(0, K_SLOT)
    def _(n):
        w1_start(n)

    pos_all = jnp.concatenate([st[i][:, 1:2] for i in range(2)], axis=0)
    cos_t, sin_t = rope_tables(pos_all)
    EARLY = (slice(0, CHUNK), slice(ROWS, ROWS + CHUNK))
    LATE = (slice(ROWS + CHUNK, PAIR), slice(CHUNK, ROWS))
    for hp in range(PAIR_HEADS):
        q = [rope(acc[0, :, span(h * LANES)], cos_t, sin_t) for h in (2 * hp, 2 * hp + 1)]
        for half, rows in enumerate((EARLY, LATE)):
            qt[half, :, span(hp * LANES)] = jnp.concatenate([v[r] for v in q for r in rows], axis=0).T.astype(BF16)

    own_plane_there()
    ml[:, 0] = jnp.full((2, SUBLANES, QL), NEG_BIG, F32)
    ml[:, 1] = jnp.zeros((2, SUBLANES, QL), F32)
    acc[:2, :, :QL] = jnp.zeros((2, HEAD_DIM, QL), F32)
    row_of = iota(PAIR, LANES, 0)
    r64 = lax.rem(iota(PAIR, LANES, 1), ROWS)

    def row_positions(rows):
        src = jnp.where(r64 < CHUNK, r64 + rows[0].start, r64 + (rows[1].start - CHUNK))
        return jnp.sum(jnp.where(row_of == src, pos_all, 0.0), axis=0, keepdims=True).astype(jnp.int32)

    pos_e, pos_l = row_positions(EARLY), row_positions(LATE)

    def natural(late, c):
        return jnp.where(late, SEQ - ROWS * (c + 1), ROWS * c)

    def step(s):
        near = s < NEAR
        r = lax.div(s - NEAR, 2)
        late_q = jnp.where(near, s >= 2, r >= cz)
        late_k = jnp.where(near, lax.div(s, 2) == 1, late_q & (r < SIDE - 1))
        dz = jnp.where(near, 0, jnp.where(late_q, jnp.where(r < SIDE - 1, r - cz + 1, r - 2), SIDE - 1 - r))
        lanes = span((late_k.astype(jnp.int32) * SIDE + dz) * LANES)
        return late_q, late_k, dz, lax.rem(s, 2) * 2, lanes

    def product(s, buf):
        late_q, late_k, dz, dy, lanes = step(s)
        q = qt[late_q.astype(jnp.int32)]
        row_nat = natural(late_q, chip) + r64[:1]
        row_first = row_nat - jnp.where(late_q, pos_l, pos_e)
        plane = lax.rem(cz + dz, SIDE) * SIDE
        u = iota(ROWS, 1, 0)
        tops = [jnp.full((SUBLANES, LANES), NEG_BIG, F32)] * SIDE
        for part in range(2):
            keys = w1[K_SLOT, dy + part, :, :, lanes].reshape(SIDE * ROWS, LANES)
            row_y = (plane + lax.rem(cy + dy + part, SIDE)) * SIDE
            scores = dot(keys, q)
            for i in range(SIDE):
                key_nat = natural(late_k, row_y + lax.rem(cx + i, SIDE)) + u
                visible = (key_nat >= row_first) & (key_nat <= row_nat)
                rows = slice(i * ROWS, (i + 1) * ROWS)
                for l in range(SIDE):
                    tile = jnp.where(visible, scores[rows, l * LANES:(l + 1) * LANES], NEG_BIG)
                    gacc[rows, span(SCORE_BUFS[buf] + part * QL + l * LANES)] = tile
                    for r in range(0, ROWS, SUBLANES):
                        tops[l] = jnp.maximum(tops[l], tile[r:r + SUBLANES])
        mx[buf] = jnp.concatenate(tops, axis=1)

    def soften(s, buf):
        late_q, _, _, dy, lanes = step(s)
        qh = late_q.astype(jnp.int32)
        m_old = ml[qh, 0, :1]
        m_new = jnp.maximum(m_old, jnp.max(mx[buf], axis=0, keepdims=True))
        shift = m_new * EXP_SCALE
        p = jnp.concatenate([jnp.exp2(gacc[:, span(SCORE_BUFS[buf] + i * QL, QL)] * EXP_SCALE - shift) for i in range(2)], axis=0)
        alpha = jnp.exp2((m_old - m_new) * EXP_SCALE)
        ml[qh, 0, :1] = m_new
        ml[qh, 1, :1] = ml[qh, 1, :1] * alpha + jnp.sum(p, axis=0, keepdims=True)
        vals = w1[K_SLOT + 1, pl.ds(dy, 2), :, :, lanes].reshape(2 * SIDE * ROWS, LANES)
        pv = lax.dot_general(vals, p.astype(BF16), (((0,), (0,)), ((), ())), preferred_element_type=F32)
        acc[qh, :, :QL] = acc[qh, :, :QL] * alpha + pv

    product(0, 0)

    @pl.loop(0, STEPS // 2)
    def _(i):
        @pl.when(i == NEAR // 2)
        def _():
            all_there()
            product(NEAR, 0)

        product(2 * i + 1, 1)
        soften(2 * i, 0)
        product(jnp.where((i == NEAR // 2 - 1) | (i == STEPS // 2 - 1), 0, 2 * i + 2), 0)
        soften(2 * i + 1, 1)

    for hp in range(PAIR_HEADS):
        for half, rows in enumerate((EARLY, LATE)):
            o = (acc[half, :, span(hp * LANES)] / ml[half, 1, :1, span(hp * LANES)]).T.astype(BF16)
            for u in range(2):
                for i, r in enumerate(rows):
                    obuf[core, r, span((2 * hp + u) * LANES)] = o[ROWS * u + CHUNK * i:ROWS * u + CHUNK * (i + 1)]
    o_copy = to_sib(obuf.at[core], obuf.at[core], os_sem, or_sem)
    o_copy.start()
    each(range(len(SENDS)), 'send', sent)
    for n in range(K_SLOT, N1):
        w1_start(n)

    def o_part(n, own):
        group = core if own else other
        places = range(2) if own else range(2, O_WIDE)
        slots = [w2_wait(Q_TRIPS + O_WIDE * n + u) for u in places]

        def part(cols):
            terms = [dot(obuf[group, :, u % 2 * KC:(u % 2 + 1) * KC], w2[s, :, :, :, cols].reshape(KC, QL)) for u, s in zip(places, slots)]
            if not own:
                for h in range(2):
                    w = bbuf[:, span((2 * n + h) * NB + cols.start, QL)]
                    terms.append(dot(obuf[group, :, span(KC + h * PAIR * 2, PAIR * 2)], w))
            return sum(terms)

        return part

    def o_block(n, parts):
        total = jnp.zeros((PAIR, LANES), F32)
        for h in range(2):
            o_spare(n, h).wait()
        for b in range(0, NB, QL):
            out = sum(p(slice(b, b + QL)) for p in parts)
            cols = span(own_col(n * NB) + b, QL)
            h = (x128[:, cols].astype(F32) + out).astype(BF16)
            x128[:, cols] = h
            hf = h.astype(F32)
            for u in range(0, QL, LANES):
                total = total + hf[:, u:u + LANES] * hf[:, u:u + LANES]
        ss[core] += total
        for u in range(O_WIDE):
            w2_start(Q_TRIPS + O_WIDE * n + u + N2)

    ss[core] = jnp.zeros((PAIR, LANES), F32)
    first = o_part(0, True)
    for b in range(0, NB, QL):
        acc[0, :, b:b + QL] = first(slice(b, b + QL))
    o_copy.wait()
    o_block(0, [lambda cols: acc[0, :, cols], o_part(0, False)])

    @pl.loop(1, BLOCKS_N)
    def _(n):
        o_block(n, [o_part(n, True), o_part(n, False)])

    for dim, k in NEIGHBOURS:
        for c in range(2):
            pl.semaphore_signal(free_sem, device_id={'cp': peer(dim, SIDE - k, c)}, device_id_type=MESH)
    ss_copy = to_sib(ss.at[core], ss.at[core], sss_sem, ssr_sem)
    ss_copy.start()
    gacc[...] = jnp.zeros_like(gacc)
    acc[...] = jnp.zeros_like(acc)
    ss_copy.wait()
    inv_h = lax.rsqrt(jnp.sum(ss[0] + ss[1], axis=1, keepdims=True) / MODEL + NORM_EPS)

    def b_copy(i, col=own_col):
        part = bbuf.at[pair_rows, span(col(i * BC), BC)]
        return to_sib(part, part, bs_sem.at[i], br_sem.at[i])

    def n_copy(cross, i, g):
        dim, k = NEIGHBOURS[g]
        cols = span(own_col(i * BC), BC)
        return remote(bbuf.at[pl.ds(g * GROUP, GROUP), cols], bbuf.at[pl.ds(PAIR + g * GROUP, GROUP), cols],
                      ns_sem.at[cross, i, g], nr_sem.at[cross, i, g], peer(dim, k, other if cross else core))

    def n_arrival(cross, i, g):
        dim, k = NEIGHBOURS[g]
        dst = bbuf.at[pl.ds(PAIR + g * GROUP, GROUP), span((sib_col if cross else own_col)(i * BC), BC)]
        return remote(dst, dst, ns_sem.at[cross, i, g], nr_sem.at[cross, i, g], peer(dim, SIDE - k, other if cross else core))

    pl.semaphore_wait(free_sem, 2 * len(NEIGHBOURS))

    @pl.loop(0, BP)
    def _(i):
        for j in range(BC // LANES):
            tile = lax.div(own_col(i * BC), LANES) + j
            cols = span(tile * LANES)
            bbuf[pair_rows, cols] = (x128[:, cols].astype(F32) * inv_h * gains[1, pl.ds(tile, 1), :]).astype(BF16)
        for g in GROUPS:
            n_copy(0, i, g).start()
        b_copy(i).start()

    @pl.loop(0, BP)
    def _(i):
        for g in GROUPS:
            n_copy(1, i, g).start()

    def h_copy(g):
        dim, k = NEIGHBOURS[g]
        rows = pl.ds(g * GROUP, GROUP)
        return remote(x128.at[rows, span(other_color * HALF + core * QUARTER, QUARTER)], x128.at[rows, span(other_color * HALF + other * QUARTER, QUARTER)],
                      hs_sem.at[g], hr_sem.at[g], peer(dim, k))

    def h_arrival(g):
        dim, k = NEIGHBOURS[g]
        dst = x128.at[pl.ds(g * GROUP, GROUP), span(color * HALF + other * QUARTER, QUARTER)]
        return remote(dst, dst, hs_sem.at[g], hr_sem.at[g], peer(dim, SIDE - k))

    for g in GROUPS:
        h_copy(g).start()

    def gate_up(rows, t, slots):
        parts = [(bbuf[rows, span(g_cols(t) + u * KC, KC)], s) for u, s in enumerate(slots)]

        def block(i, cols):
            return [w1[s, 2 * i:2 * i + 2, :, :, cols].reshape(KC, cols.stop - cols.start) for _, s in parts]

        def product_of(weights):
            return sum(dot(a, w) for (a, _), w in zip(parts, weights))

        for i in range(2):
            for b in range(0, FFQ - LANES, QL):
                gacc[rows, i * FFQ + b:i * FFQ + b + QL] += product_of(block(i, slice(b, b + QL)))
        last = slice(FFQ - LANES, FFQ)
        pair = product_of([jnp.concatenate(w, axis=1) for w in zip(block(0, last), block(1, last))])
        gacc[rows, last] += pair[:, :LANES]
        gacc[rows, 2 * FFQ - LANES:] += pair[:, LANES:]

    def refill(t):
        for u in range(2):
            w1_start(2 * t + u + N1)

    @pl.loop(0, PRE)
    def _(t):
        gate_up(slice(0, PAIR), t, [w1_wait(2 * t + u) for u in range(2)])

    @pl.loop(0, PRE)
    def _(t):
        for g in GROUPS:
            n_arrival(0, t, g).wait_recv()
        gate_up(slice(PAIR, 2 * PAIR), t, [2 * t + u for u in range(2)])
        refill(t)

    @pl.loop(PRE, G_TRIPS)
    def _(t):
        @pl.when(t < BP)
        def _():
            for g in GROUPS:
                n_arrival(0, t, g).wait_recv()

        @pl.when(t >= BP)
        def _():
            b_copy(t - BP, sib_col).wait_recv()
            for g in GROUPS:
                n_arrival(1, t - BP, g).wait_recv()

        gate_up(slice(0, 2 * PAIR), t, [w1_wait(2 * t + u) for u in range(2)])
        refill(t)

    def gated(rows):
        @pl.loop(0, FFQ // LANES)
        def _(j):
            g = gacc[rows, span(j * LANES)]
            mbuf[rows, span(hidden + j * LANES)] = (g * (1.0 / (1.0 + jnp.exp(-g))) * gacc[rows, span(FFQ + j * LANES)]).astype(BF16)

    def kind_rows(kind, g):
        return pl.ds(kind * PAIR + g * GROUP, GROUP)

    def m_send(kind, g):
        dim, k = NEIGHBOURS[g]
        cols = span(hidden, FFQ)
        return remote(mbuf.at[kind_rows(kind, g), cols], mbuf.at[kind_rows(1 - kind, g), cols], nms_sem.at[kind, g], nmr_sem.at[1 - kind, g],
                      peer(dim, k if kind == 0 else SIDE - k))

    def m_place(kind, g, c):
        return mbuf.at[kind_rows(kind, g), span(other_color * FFH + c * FFQ, FFQ)]

    def m_arrival(kind, g):
        dim, k = NEIGHBOURS[g]
        dst = m_place(kind, g, core)
        return remote(dst, dst, nms_sem.at[kind, g], nmr_sem.at[kind, g], peer(dim, k if kind == 0 else SIDE - k))

    def m_pass_on(kind, g, c=core):
        part = m_place(kind, g, c)
        return to_sib(part, part, fms_sem.at[kind, g], fmr_sem.at[kind, g])

    def m_copy(of_core):
        part = mbuf.at[:, span(color * FFH + of_core * FFQ, FFQ)]
        return to_sib(part, part, ms_sem, mr_sem)

    for kind in (1, 0):
        gated(pl.ds(kind * PAIR, PAIR))
        for g in GROUPS:
            m_send(kind, g).start()
    m_copy(core).start()

    def d_rows(rows, kk):
        return mbuf[rows, span(d_chunk(kk) * KC, KC)]

    def first_product(kk, weights):
        a = d_rows(slice(0, 2 * PAIR), kk)
        for n, weight in enumerate(weights):
            for b in range(0, NB, QL):
                out = dot(a, weight(slice(b, b + QL)))
                for r in range(2):
                    acc[2 * n + r, :, b:b + QL] += out[r * PAIR:(r + 1) * PAIR]

    def of_wide(slot):
        return lambda cols: w2[slot, :, :, :, cols].reshape(KC, QL)

    def of_narrow(slot):
        return lambda cols: w1[slot, cols.start // BC * 2:cols.start // BC * 2 + 2, :, :, cols.start % BC:cols.start % BC + QL].reshape(KC, QL)

    @pl.loop(0, SIDE)
    def _(kk):
        @pl.when(kk == 2)
        def _():
            m_copy(core).wait_send()
            m_copy(other).wait_recv()

        places = [Q_TRIPS + O_SLOTS + 2 * kk + u for u in range(2)]
        first_product(kk, [of_wide(w2_wait(n)) for n in places])
        for n in places:
            w2_start(n + N2)

    for kk in range(SIDE, D_OWN):
        places = [G_SLOTS + 2 * (kk - SIDE) + u for u in range(2)]
        first_product(kk, [of_narrow(w1_wait_down(n)) for n in places])
        for n in places:
            if n + N1 < G_SLOTS + len(D_NARROW):
                w1_start(n + N1)

    @pl.loop(0, BP)
    def _(i):
        b_copy(i).wait_send()
        for cross in range(2):
            for g in GROUPS:
                n_copy(cross, i, g).wait_send()

    for kind in (1, 0):
        for g in GROUPS:
            m_arrival(kind, g).wait_recv()
            m_pass_on(kind, g).start()
    for g in GROUPS:
        h_copy(g).wait_send()
        h_arrival(g).wait_recv()
    for kind in range(2):
        for g in GROUPS:
            m_pass_on(kind, g).wait_send()
            m_pass_on(kind, g, other).wait_recv()

    def d_slots(n, wait):
        found = []
        for i in range(D_FIRST + n * D_REST, D_FIRST + (n + 1) * D_REST):
            if i in D_WIDE:
                place = Q_TRIPS + O_SLOTS + D_WIDE.index(i)
                found.append((i, w2, place % N2))
                if wait:
                    w2_wait(place)
            else:
                place = G_SLOTS + D_NARROW.index(i)
                found.append((i, w1, place % N1))
                if wait:
                    w1_wait_down(place)
        return found

    def d_cols(n, h, to_core=core, of_color=color):
        return span(of_color * HALF + to_core * QUARTER + n * NB + h * BC, BC)

    def second_product(kind, n, h, found):
        for b in range(0, BC, QL):
            out = acc[2 * n + kind, :, span(h * BC + b, QL)]
            for i, ring, slot in found:
                if ring is w2:
                    weight = w2[slot, :, :, :, span(h * BC + b, QL)]
                else:
                    weight = w1[slot, pl.ds(2 * h, 2), :, :, b:b + QL]
                out += dot(d_rows(pl.ds(kind * PAIR, PAIR), d_place(i)[1]), weight.reshape(KC, QL))
            place = n * NB + h * BC + b
            residual = x128[:, span(color * HALF + (other if kind else core) * QUARTER + place, QL)]
            bbuf[pl.ds(kind * PAIR, PAIR), span(color * HALF + core * QUARTER + place, QL)] = (residual.astype(F32) + out).astype(BF16)

    def z_away(n, h, g):
        dim, k = NEIGHBOURS[g]
        dst = z_hbm.at[pl.ds(g % 2 * GROUP, GROUP), d_cols(n, h)]
        return remote(bbuf.at[kind_rows(1, g), d_cols(n, h)], dst, za_sem.at[n, h, g], zb_sem.at[core, n, h, g % 2], peer(dim, SIDE - k, g // 2))

    def z_back(c, n, h, i):
        part = z_hbm.at[pl.ds(i * GROUP, GROUP), d_cols(n, h, c, other_color)]
        return to_sib(part, part, za_sem.at[n, h, i], zb_sem.at[c, n, h, i])

    def z_local(n, h):
        return pltpu.make_async_copy(bbuf.at[own_rows, d_cols(n, h)], z_hbm.at[:, d_cols(n, h)], zl_sem.at[n, h])

    def z_remote(n, h, c=core):
        return to_sib(bbuf.at[sib_rows, d_cols(n, h, c)], z_hbm.at[:, d_cols(n, h, c)], zs_sem.at[n, h], zr_sem.at[n, h])

    for n in range(D_BLOCKS):
        found = d_slots(n, True)

        @pl.loop(0, 2)
        def _(h):
            second_product(1, n, h, found)
            for g in GROUPS:
                z_away(n, h, g).start()

    for n in range(D_BLOCKS):
        found = d_slots(n, False)

        @pl.loop(0, 2)
        def _(h):
            second_product(0, n, h, found)
            z_local(n, h).start()
            z_remote(n, h).start()

    for n in range(D_BLOCKS):
        for h in range(2):
            z_local(n, h).wait()
            z_remote(n, h).wait_send()
            z_remote(n, h, other).wait_recv()
            for g in GROUPS:
                z_away(n, h, g).wait_send()
            for c in range(2):
                for i in range(2):
                    z_back(c, n, h, i).wait_recv()
    for kind in range(2):
        for g in GROUPS:
            m_send(kind, g).wait_send()
    for s in stores:
        s.wait()


def deliver_kernel(z_in, k_in, v_in, z_out, k_out, v_out, zb, kb, in_sem, out_sem):
    moves = [(k_in, kb.at[0], k_out), (v_in, kb.at[1], v_out)]
    for first in range(0, MODEL, DELIVER):
        cols = span(first, DELIVER)
        moves.append((z_in.at[:, cols], zb.at[:, cols], z_out.at[:, cols]))
    moves = [(pltpu.make_async_copy(src, mid, in_sem.at[i]), pltpu.make_async_copy(mid, dst, out_sem.at[i])) for i, (src, mid, dst) in enumerate(moves)]
    for come, _ in moves:
        come.start()
    for come, go in moves:
        come.wait()
        go.start()
    for _, go in moves:
        go.wait()


def solution(mesh):
    def device_fn(x_loc, seg_loc, pos_loc, attn_gain, w_q, w_k, w_v, w_o, mlp_gain, w_gate, w_up, w_down):
        any_space = pl.BlockSpec(memory_space=pl.ANY)
        vmem = pl.BlockSpec(memory_space=pltpu.VMEM)

        def blocks(w):
            return w.reshape(-1, SIDE, ROWS, w.shape[1])

        def gain(g):
            return g.reshape(-1, LANES)

        z_shape, k_shape = (jax.ShapeDtypeStruct((ROWS, n), BF16) for n in (MODEL, HEAD_DIM))
        outs = (z_shape, k_shape, k_shape)
        f32_buffers = ((BLOCKS_N, PAIR, NB), (2 * PAIR, 2 * FFQ))
        stats = ((2, 2, SUBLANES, QL), (2, SUBLANES, QL))
        sems = {
            'xl': (), 'xs': (XP,), 'xr': (XP,), 'sts': (), 'str': (), 'kvw': (2, KV_PIECES), 'w1': (N1,), 'w2': (N2,),
            'gs': (len(BLOCKS), len(SENDS), len(STEPS_ALONG)), 'gr': (len(BLOCKS), len(SENDS), len(STEPS_ALONG)),
            'fs': (len(BLOCKS), len(SENDS) + 1, len(STEPS_ALONG)), 'fr': (len(BLOCKS), len(SENDS) + 1, len(STEPS_ALONG)),
            'os': (), 'or': (), 'sss': (), 'ssr': (), 'bs': (BP,), 'br': (BP,), 'ns': (2, BP, len(GROUPS)), 'nr': (2, BP, len(GROUPS)),
            'ms': (), 'mr': (), 'nms': (2, len(GROUPS)), 'nmr': (2, len(GROUPS)), 'fms': (2, len(GROUPS)), 'fmr': (2, len(GROUPS)), 'hs': (len(GROUPS),), 'hr': (len(GROUPS),),
            'za': (D_BLOCKS, 2, len(GROUPS)), 'zb': (2, D_BLOCKS, 2, 2), 'zl': (D_BLOCKS, 2), 'zs': (D_BLOCKS, 2), 'zr': (D_BLOCKS, 2), 'ko': (2,), 'spare': (BLOCKS_N, 2),
        }

        def dma(shape):
            return pltpu.SemaphoreType.DMA(shape) if shape else pltpu.SemaphoreType.DMA

        results = pl.pallas_call(
            layer_kernel,
            out_shape=outs,
            in_specs=[any_space, vmem, vmem, any_space, any_space, any_space, any_space, any_space, vmem, any_space, any_space, any_space],
            out_specs=(any_space,) * len(outs),
            scratch_shapes=[
                pltpu.VMEM((PAIR, MODEL), BF16),
                pltpu.VMEM((2 * PAIR, MODEL), BF16),
                pltpu.VMEM((N1, SIDE, SIDE, ROWS, FFQ), BF16),
                pltpu.VMEM((N2, 2, SIDE, ROWS, NB), BF16),
                *(pltpu.VMEM(s, F32) for s in f32_buffers),
                pltpu.VMEM((2, HEAD_DIM, QL), BF16),
                *(pltpu.VMEM(s, F32) for s in stats),
                pltpu.VMEM((2, PAIR, QCOLS), BF16),
                pltpu.VMEM((2 * PAIR, FF), BF16),
                pltpu.VMEM((2, ROWS, LANES), F32),
                pltpu.VMEM((2, PAIR, LANES), F32),
                pltpu.VMEM((2, ROWS, LANES), BF16),
                pltpu.VMEM((2, LANES, LANES), F32),
                *(dma(s) for s in sems.values()),
                pltpu.SemaphoreType.REGULAR,
            ],
            compiler_params=pltpu.CompilerParams(collective_id=0, has_side_effects=True, vmem_limit_bytes=67043328),
            name='layer',
        )(x_loc[0], pos_loc.reshape(1, ROWS), gain(attn_gain), blocks(w_q), blocks(w_k), blocks(w_v), blocks(w_o), w_o, gain(mlp_gain),
          blocks(w_gate), blocks(w_up), blocks(w_down))
        moves = MODEL // DELIVER + 2
        z_rows, k_rows, v_rows = pl.pallas_call(
            deliver_kernel,
            out_shape=outs,
            in_specs=[any_space] * len(outs),
            out_specs=(any_space,) * len(outs),
            scratch_shapes=[pltpu.VMEM((ROWS, MODEL), BF16), pltpu.VMEM((2, ROWS, HEAD_DIM), BF16), dma((moves,)), dma((moves,))],
            compiler_params=pltpu.CompilerParams(vmem_limit_bytes=62914560),
            name='finish',
        )(*results)
        return z_rows[None], k_rows[:, None, :], v_rows[:, None, :]

    seq_spec = P(('dp', 'cp'))
    rows_spec, cache_spec = P('dp', 'cp', None), P(('dp', 'cp'), None, None)
    return jax.shard_map(device_fn, mesh=mesh, in_specs=(rows_spec, seq_spec, seq_spec) + (P(),) * 9, out_specs=(rows_spec, cache_spec, cache_spec), check_vma=False)
```

```python
import functools
import math

import jax
import jax.numpy as jnp
from jax import lax
from jax.experimental import pallas as pl
from jax.experimental.pallas import tpu as pltpu
from jax.sharding import PartitionSpec as P

LANES = 128
SUBLANES = 8
SIDE = 4
MODEL = 16384
HALF = MODEL // 2
QUARTER = MODEL // 4
HEADS = 16
PAIR_HEADS = HEADS // 4
HEAD_DIM = LANES
QCOLS = HEADS * HEAD_DIM // 2
FF = 6656
FFH = FF // 2
FFQ = FF // 4
ROWS = 64
CHUNK = 32
PAIR = 2 * ROWS
SEQ = 8192
ROPE_THETA = 500000.0
ROPE_FACTOR = 8.0
LOW_FREQ = 1.0
HIGH_FREQ = 4.0
ORIG_CTX = 8192.0
NORM_EPS = 1e-5
NEG_BIG = -1e30
EXP_SCALE = HEAD_DIM ** -0.5 * math.log2(math.e)

KC = 512
NB = 2048
N1 = 6
K_SLOT = 4
N2 = 9
BLOCKS_N = HALF // NB
Q_TRIPS = MODEL // (2 * KC)
O_CHUNKS = HEADS * HEAD_DIM // KC
O_WIDE = O_CHUNKS - 1
O_SLOTS = BLOCKS_N * O_WIDE
D_CHUNKS = FF // KC
D_OWN = D_CHUNKS // 2
D_REST = D_CHUNKS - D_OWN
D_BLOCKS = QUARTER // NB
D_FIRST = D_OWN * D_BLOCKS
D_SLOTS = D_CHUNKS * D_BLOCKS
D_NARROW = (8, 9, 10, 11, 13, 14, 23, 24, 25)
G_SLOTS = MODEL // KC
G_TRIPS = G_SLOTS // 2
G_NARROW = G_SLOTS - 2
BC = 2 * KC
BP = HALF // BC
XP = 4
PIECES_PER_SLOT = FFQ // LANES
KV_PIECES = MODEL // KC
KV_UNROLL = 8
HOOK_B, HOOK_C = 0, 11
PRE = 3
WIDE_D = Q_TRIPS + O_SLOTS
D_EARLY = 5
WIDE_G = WIDE_D + D_EARLY
WIDE_LATE = WIDE_G + N2
D_LATE = 3
D_KEPT = 12
QL = 512
SCORE_BUFS = (0, 2 * QL)
NEAR = 6
STEPS = 18
DELIVER = 2048
NEIGHBOURS = (('x', 1), ('x', 3), ('y', 1), ('y', 3))
GROUPS = range(len(NEIGHBOURS))
GROUP = PAIR // len(NEIGHBOURS)

MESH = pl.DeviceIdType.MESH
F32 = jnp.float32
BF16 = jnp.bfloat16
BLOCKS = (((0, 1), 0, 'yzx'), ((1, 1), 0, 'zxy'), ((0, 2), 1, 'xyz'))
OWN = (0, 0, 0)
SENDS = ((OWN, 0), (OWN, 1), (OWN, 2), ((1, 0, 0), 1), ((1, 0, 0), 2), ((0, 1, 0), 2), ((1, 1, 0), 2))
ROUNDS = ((0, 1, 2), (3, 4, 5), (6,))
STEPS_ALONG = (1, 2, 3)
BOTH = range(2)


def dot(a, b):
    return jnp.dot(a, b, preferred_element_type=F32)


def span(first, count=LANES):
    return pl.ds(pl.multiple_of(first, LANES), count)


def iota(rows, cols, dim):
    return lax.broadcasted_iota(jnp.int32, (rows, cols), dim)


def rope_tables(pos):
    lane = iota(SUBLANES, HEAD_DIM, 1)
    j = lax.rem(lane, HEAD_DIM // 2).astype(F32)
    inv_freq = jnp.exp(j * (-2.0 / HEAD_DIM * math.log(ROPE_THETA)))
    wavelen = (2.0 * math.pi) / inv_freq
    smooth = jnp.clip((ORIG_CTX / wavelen - LOW_FREQ) / (HIGH_FREQ - LOW_FREQ), 0.0, 1.0)
    freq = ((1.0 - smooth) * inv_freq / ROPE_FACTOR + smooth * inv_freq)[:1]
    angle = pos * freq
    sign = jnp.where(lane[:1] < HEAD_DIM // 2, -1.0, 1.0)
    return jnp.cos(angle), jnp.sin(angle) * sign


def rope(t, cos_t, sin_t):
    return t * cos_t + pltpu.roll(t, HEAD_DIM // 2, 1) * sin_t


def layer_kernel(x_hbm, pos_ref, ag_ref, wq, wk, wv, wo, wo_rows, mg_ref, wg, wu, wd,
                 z_hbm, k_out, v_out,
                 x128, bbuf, w1, w2, acc, gacc, qt, ml, mx, obuf, mbuf, st, ss, kst, gains,
                 xl_sem, xs_sem, xr_sem, sts_sem, str_sem, kvw_sem, w1_sem, w2_sem, gs_sem, gr_sem, fs_sem, fr_sem,
                 os_sem, or_sem, sss_sem, ssr_sem, bs_sem, br_sem, ns_sem, nr_sem, ms_sem, mr_sem, nms_sem, nmr_sem, fms_sem, fmr_sem, hs_sem, hr_sem,
                 za_sem, zb_sem, zl_sem, zs_sem, zr_sem, ko_sem, spare_sem, free_sem):
    me = lax.axis_index('cp')
    core = lax.rem(me, 2)
    chip = lax.div(me, 2)
    coords = {'x': lax.rem(chip, SIDE), 'y': lax.rem(lax.div(chip, SIDE), SIDE), 'z': lax.div(chip, SIDE * SIDE)}
    cx, cy, cz = coords['x'], coords['y'], coords['z']
    other = 1 - core
    sib = me + other - core
    color = lax.rem(cx + cy + cz, 2)
    hidden = pl.multiple_of(color * FFH + core * FFQ, LANES)

    def peer(dim, k, to_core=core):
        c = dict(coords)
        c[dim] = lax.rem(c[dim] + k, SIDE)
        return ((c['z'] * SIDE + c['y']) * SIDE + c['x']) * 2 + to_core

    def remote(src, dst, s, r, dev):
        return pltpu.make_async_remote_copy(src, dst, s, r, device_id={'cp': dev}, device_id_type=MESH)

    def to_sib(src, dst, s, r):
        return remote(src, dst, s, r, sib)

    own_rows = pl.ds(pl.multiple_of(core * ROWS, ROWS), ROWS)
    sib_rows = pl.ds(pl.multiple_of(other * ROWS, ROWS), ROWS)
    pair_rows = pl.ds(0, PAIR)

    def col_of(c, v):
        return lax.div(v, QUARTER) * HALF + c * QUARTER + lax.rem(v, QUARTER)

    def own_col(v):
        return col_of(core, v)

    def sib_col(v):
        return col_of(other, v)

    def w_rows(first):
        return pl.ds(lax.div(first, KC // 2), 2)

    def kv_dst(c, i):
        return w1.at[lax.div(c, PIECES_PER_SLOT), pl.ds(2 * i, 2), :, :, span(lax.rem(c, PIECES_PER_SLOT) * LANES)]

    def kv_copy(c, i):
        return pltpu.make_async_copy((wk, wv)[i].at[w_rows(c * KC)], kv_dst(c, i), kvw_sem.at[i, c])

    def o_chunk(u):
        return lax.rem(u + 2 * core, O_CHUNKS)

    def o_spare(n, h):
        rows = pl.ds(o_chunk(O_WIDE) * KC + h * PAIR * 2, PAIR * 2)
        return pltpu.make_async_copy(wo_rows.at[rows, span(own_col(n * NB), NB)], bbuf.at[:, span((2 * n + h) * NB, NB)], spare_sem.at[n, h])

    def d_place(i):
        first = i < D_FIRST
        n = jnp.where(first, lax.rem(i, D_BLOCKS), lax.div(i - D_FIRST, D_REST))
        return n, jnp.where(first, lax.div(i, D_BLOCKS), D_OWN + lax.rem(i - D_FIRST, D_REST))

    def d_chunk(kk):
        mine = color * D_REST + jnp.where(core == 0, kk, D_OWN - 1 - kk)
        return jnp.where(kk < D_OWN, mine, jnp.where(kk == D_OWN, D_OWN, (other_color * D_REST) + kk - D_REST))

    def d_source(i, first, count):
        n, kk = d_place(i)
        return wd.at[w_rows(d_chunk(kk) * KC), :, :, span(color * HALF + core * QUARTER + n * NB + first, count)]

    other_color = 1 - color

    def w2_start(n):
        slot = lax.rem(n, N2)

        @pl.when(n < Q_TRIPS)
        def _():
            for h in BOTH:
                src = wq.at[w_rows(n * (2 * KC) + h * KC), :, :, span(core * QCOLS, QCOLS)]
                pltpu.make_async_copy(src, w2.at[slot, :, :, :, pl.ds(h * QCOLS, QCOLS)], w2_sem.at[slot]).start()

        @pl.when((n >= Q_TRIPS) & (n < Q_TRIPS + O_SLOTS))
        def _():
            i = n - Q_TRIPS
            src = wo.at[w_rows(o_chunk(lax.rem(i, O_WIDE)) * KC), :, :, span(own_col(lax.div(i, O_WIDE) * NB), NB)]
            pltpu.make_async_copy(src, w2.at[slot], w2_sem.at[slot]).start()

        @pl.when((n >= WIDE_G) & (n < WIDE_D + N2))
        def _():
            u = n - WIDE_G
            rows = w_rows(g_cols(PRE) + lax.div(u, 2) * KC)
            for i, w in enumerate((wg, wu)):
                @pl.when(lax.rem(u, 2) == i)
                def _():
                    pltpu.make_async_copy(w.at[rows, :, :, span(hidden, FFQ)], w2.at[slot, :, :, :, pl.ds(0, FFQ)], w2_sem.at[slot]).start()

        @pl.when((n >= WIDE_D) & ((n < WIDE_G) | (n >= WIDE_D + N2)))
        def _():
            late = n - (WIDE_D + N2) + D_KEPT + D_LATE
            i = jnp.where(n < WIDE_G, n - WIDE_D, jnp.where(n < WIDE_LATE, late, jnp.where(n < WIDE_LATE + D_LATE, n - WIDE_LATE + D_EARLY, jnp.where(
                n == WIDE_LATE + D_LATE, D_KEPT, n - (WIDE_LATE + N2) + D_KEPT + D_LATE + D_EARLY))))
            pltpu.make_async_copy(d_source(i, 0, NB), w2.at[slot], w2_sem.at[slot]).start()

    def d_wide(i):
        if isinstance(i, int) and i >= D_KEPT:
            return WIDE_LATE + D_LATE if i == D_KEPT else i - D_KEPT - D_LATE + (WIDE_D + N2 if i < D_KEPT + D_LATE + D_EARLY else WIDE_LATE + N2 - D_EARLY)
        return jnp.where(i < D_EARLY, WIDE_D + i, WIDE_LATE - D_EARLY + i)

    def w2_wait(n):
        slot = lax.rem(n, N2)
        pltpu.make_async_copy(wo.at[w_rows(0), :, :, span(0, NB)], w2.at[slot], w2_sem.at[slot]).wait()
        return slot

    def wide(slot):
        return w2[slot].reshape(KC, NB)

    def g_cols(t):
        return pl.multiple_of(col_of(jnp.where(t < BP, core, other), lax.rem(t, BP) * BC), BC)

    def w1_start(n):
        slot = lax.rem(n, N1)

        @pl.when(n < G_NARROW)
        def _():
            t = lax.div(n, 2)
            first = g_cols(jnp.where(t < PRE, t, t + 1))
            for i, w in enumerate((wg, wu)):
                src = w.at[w_rows(first + lax.rem(n, 2) * KC), :, :, span(hidden, FFQ)]
                pltpu.make_async_copy(src, w1.at[slot, pl.ds(2 * i, 2)], w1_sem.at[slot]).start()

        @pl.when(n >= G_NARROW)
        def _():
            u = n - G_NARROW
            i = jnp.where(u < SIDE, D_NARROW[0] + u, jnp.where(u < N1, D_NARROW[SIDE] - SIDE + u, D_NARROW[N1] - N1 + u))
            for h in BOTH:
                pltpu.make_async_copy(d_source(i, h * BC, BC), w1.at[slot, pl.ds(2 * h, 2), :, :, span(0, BC)], w1_sem.at[slot]).start()

    def w1_wait(n):
        slot = lax.rem(n, N1)
        pltpu.make_async_copy(wg.at[pl.ds(0, SIDE), :, :, span(0, FFQ)], w1.at[slot], w1_sem.at[slot]).wait()
        return slot

    def w1_wait_down(n):
        slot = lax.rem(n, N1)
        pltpu.make_async_copy(wd.at[pl.ds(0, SIDE), :, :, span(0, BC)], w1.at[slot, :, :, :, span(0, BC)], w1_sem.at[slot]).wait()
        return slot

    x_local = pltpu.make_async_copy(x_hbm, x128.at[own_rows, :], xl_sem)
    x_local.start()
    barrier = pltpu.get_barrier_semaphore()
    greeted = [sib] + [peer(dim, k) for dim in 'xyz' for k in STEPS_ALONG] + [peer(dim, k, other) for dim, k in NEIGHBOURS]
    for dev in greeted:
        pl.semaphore_signal(barrier, device_id={'cp': dev}, device_id_type=MESH)

    @pl.loop(0, KV_PIECES)
    def _(c):
        for i in BOTH:
            kv_copy(c, i).start()

    def x_copy(i):
        cols = span(i * (MODEL // XP), MODEL // XP)
        return to_sib(x_hbm.at[:, cols], x128.at[own_rows, cols], xs_sem.at[i], xr_sem.at[i])

    eye = iota(ROWS, ROWS, 0) == iota(ROWS, ROWS, 1)
    pos_own = jnp.sum(jnp.where(eye, jnp.broadcast_to(pos_ref[...].astype(F32), (ROWS, ROWS)), 0.0), axis=1, keepdims=True)
    cos_own, sin_own = rope_tables(pos_own)
    gains[0] = ag_ref[...].astype(F32)
    gains[1] = mg_ref[...].astype(F32)

    x_local.wait()

    def square_sum(i, part):
        for u in range(SUBLANES):
            v = x128[own_rows, span(i * BC + u * LANES)].astype(F32)
            part = part + v * v
        return part

    part = lax.fori_loop(0, MODEL // BC, square_sum, jnp.zeros((ROWS, LANES), F32))
    inv_own = lax.rsqrt(jnp.sum(part, axis=1, keepdims=True) / MODEL + NORM_EPS)
    pl.semaphore_wait(barrier, len(greeted))
    for i in range(XP):
        x_copy(i).start()
    st[core] = jnp.where(iota(ROWS, LANES, 1) == 0, inv_own, pos_own)
    st_copy = to_sib(st.at[core], st.at[core], sts_sem, str_sem)
    st_copy.start()

    def normalize(rows, inv, lo, hi):
        @pl.loop(lo, hi)
        def _(i):
            for u in range(SUBLANES):
                tile = i * SUBLANES + u
                cols = span(tile * LANES)
                bbuf[rows, cols] = (x128[rows, cols].astype(F32) * inv * gains[0, pl.ds(tile, 1), :]).astype(BF16)

    normalize(own_rows, inv_own, 0, MODEL // BC)

    def kv_trip(i, total):
        places = [i * KV_UNROLL + u for u in range(KV_UNROLL)]
        for c in places:
            for j in BOTH:
                kv_copy(c, j).wait()
        for c in places:
            w = jnp.concatenate([kv_dst(c, j)[...].reshape(KC, LANES) for j in BOTH], axis=1)
            total = total + dot(bbuf[own_rows, span(c * KC, KC)], w)
        return total

    kv_raw = lax.fori_loop(0, KV_PIECES // KV_UNROLL, kv_trip, jnp.zeros((ROWS, 2 * LANES), F32))
    @pl.loop(0, N2)
    def _(n):
        w2_start(n)

    r0 = (pl.multiple_of(core * CHUNK, CHUNK), pl.multiple_of(other * CHUNK, CHUNK))
    stores = []
    for i, (t, out) in enumerate(((rope(kv_raw[:, :LANES], cos_own, sin_own), k_out), (kv_raw[:, LANES:], v_out))):
        t = t.astype(BF16)
        w1[K_SLOT + i, 0, 0, pl.ds(r0[0], CHUNK), :LANES] = t[:CHUNK]
        w1[K_SLOT + i, 0, 0, pl.ds(r0[1], CHUNK), span(SIDE * LANES)] = t[CHUNK:]
        kst[i] = t
        stores.append(pltpu.make_async_copy(kst.at[i], out, ko_sem.at[i]))
        stores[i].start()

    def region(b, spec, dim=None, place=None, rows=0):
        slots, half, dims = BLOCKS[b]

        def at(d):
            first, count = (place, 1) if d == dim else (1, SIDE - 1) if spec[dims.index(d)] else (0, 1)
            return first, count

        first, count = at('z')
        lanes = pl.ds((half * SIDE + first) * LANES, count * LANES)
        rows = pl.ds(r0[half if rows == 0 else 1 - half], CHUNK)
        return w1.at[pl.ds(K_SLOT + slots[0], slots[1]), pl.ds(*at('y')), pl.ds(*at('x')), rows, lanes]

    def gather_copy(b, n, k):
        spec, along = SENDS[n]
        dim = BLOCKS[b][2][along]
        return remote(region(b, spec), region(b, spec, dim, SIDE - k), gs_sem.at[b, n, k - 1], gr_sem.at[b, n, k - 1], peer(dim, k))

    def forward(b, n, k, rows=0):
        spec, along = SENDS[n]
        part = region(b, spec, BLOCKS[b][2][along], SIDE - k, rows)
        return to_sib(part, part, fs_sem.at[b, n, k - 1], fr_sem.at[b, n, k - 1])

    def own_forward(b, rows=0):
        part = region(b, OWN, rows=rows)
        return to_sib(part, part, fs_sem.at[b, len(SENDS), 0], fr_sem.at[b, len(SENDS), 0])

    def each(sends, side, action):
        for n in sends:
            for b in range(len(BLOCKS)):
                for k in STEPS_ALONG:
                    if BLOCKS[b][1] == 1 and BLOCKS[b][2][SENDS[n][1]] == 'z':
                        pl.when(cz + k >= SIDE if side == 'send' else cz < k)(functools.partial(action, b, n, k))
                    else:
                        action(b, n, k)

    def send(b, n, k):
        gather_copy(b, n, k).start()

    def sent(b, n, k):
        gather_copy(b, n, k).wait_send()

    def receive(b, n, k):
        gather_copy(b, n, k).wait_recv()

    def pass_on(b, n, k):
        forward(b, n, k).start()

    def receive_pass_on(b, n, k):
        receive(b, n, k)
        pass_on(b, n, k)

    def passed(b, n, k):
        forward(b, n, k).wait_send()
        forward(b, n, k, 1).wait_recv()

    each(ROUNDS[0], 'send', send)
    for b in range(len(BLOCKS)):
        own_forward(b).start()

    def second_round():
        each(ROUNDS[0][:2], 'recv', receive)
        each(ROUNDS[1], 'send', send)
        each(ROUNDS[0][:2], 'recv', pass_on)
        each(ROUNDS[0][2:], 'recv', receive_pass_on)

    def third_round():
        each(ROUNDS[1][:1], 'recv', receive)
        each(ROUNDS[2], 'send', send)
        each(ROUNDS[1][:1], 'recv', pass_on)

    def own_plane_there():
        each(ROUNDS[1][1:], 'recv', receive_pass_on)
        for b in range(len(BLOCKS)):
            own_forward(b).wait_send()
            own_forward(b, 1).wait_recv()
        each(ROUNDS[0] + ROUNDS[1], 'recv', passed)

    def all_there():
        each(ROUNDS[2], 'recv', receive_pass_on)
        each(ROUNDS[2], 'recv', passed)

    st_copy.wait()
    inv_sib = st[other][:, :1]
    for i in range(XP):
        x_copy(i).wait()
        normalize(sib_rows, inv_sib, i * XP, (i + 1) * XP)

    acc[0] = jnp.zeros((PAIR, NB), F32)

    @pl.loop(0, Q_TRIPS)
    def _(i):
        pl.when(i == HOOK_B)(second_round)
        pl.when(i == HOOK_C)(third_round)
        w = wide(w2_wait(i))
        acc[0, :, :QCOLS] += (dot(bbuf[pair_rows, span(i * BC, KC)], w[:, :QCOLS])
                              + dot(bbuf[pair_rows, span(i * BC + KC, KC)], w[:, QCOLS:]))
        w2_start(i + N2)

    for n in range(BLOCKS_N):
        for h in BOTH:
            o_spare(n, h).start()

    @pl.loop(0, K_SLOT)
    def _(n):
        w1_start(n)

    pos_all = jnp.concatenate([st[i][:, 1:2] for i in BOTH], axis=0)
    cos_t, sin_t = rope_tables(pos_all)
    EARLY = (slice(0, CHUNK), slice(ROWS, ROWS + CHUNK))
    LATE = (slice(ROWS + CHUNK, PAIR), slice(CHUNK, ROWS))
    for hp in range(PAIR_HEADS):
        q = [rope(acc[0, :, span(h * LANES)], cos_t, sin_t) for h in (2 * hp, 2 * hp + 1)]
        for half, rows in enumerate((EARLY, LATE)):
            qt[half, :, span(hp * LANES)] = jnp.concatenate([v[r] for v in q for r in rows], axis=0).T.astype(BF16)

    own_plane_there()
    ml[:, 0] = jnp.full((2, SUBLANES, QL), NEG_BIG, F32)
    ml[:, 1] = jnp.zeros((2, SUBLANES, QL), F32)
    acc[:2, :, :QL] = jnp.zeros((2, HEAD_DIM, QL), F32)
    row_of = iota(PAIR, LANES, 0)
    r64 = lax.rem(iota(PAIR, LANES, 1), ROWS)

    def row_positions(rows):
        src = jnp.where(r64 < CHUNK, r64 + rows[0].start, r64 + (rows[1].start - CHUNK))
        return jnp.sum(jnp.where(row_of == src, pos_all, 0.0), axis=0, keepdims=True).astype(jnp.int32)

    pos_e, pos_l = row_positions(EARLY), row_positions(LATE)

    def natural(late, c):
        return jnp.where(late, SEQ - ROWS * (c + 1), ROWS * c)

    def step(s):
        near = s < NEAR
        r = lax.div(s - NEAR, 2)
        late_q = jnp.where(near, s >= 2, r >= cz)
        late_k = jnp.where(near, lax.div(s, 2) == 1, late_q & (r < SIDE - 1))
        dz = jnp.where(near, 0, jnp.where(late_q, jnp.where(r < SIDE - 1, r - cz + 1, r - 2), SIDE - 1 - r))
        lanes = span((late_k.astype(jnp.int32) * SIDE + dz) * LANES)
        return late_q, late_k, dz, lax.rem(s, 2) * 2, lanes

    def product(s, buf):
        late_q, late_k, dz, dy, lanes = step(s)
        q = qt[late_q.astype(jnp.int32)]
        row_nat = natural(late_q, chip) + r64[:1]
        row_first = row_nat - jnp.where(late_q, pos_l, pos_e)
        plane = lax.rem(cz + dz, SIDE) * SIDE
        u = iota(ROWS, 1, 0)
        tops = [jnp.full((SUBLANES, LANES), NEG_BIG, F32)] * SIDE
        for part in BOTH:
            keys = w1[K_SLOT, dy + part, :, :, lanes].reshape(SIDE * ROWS, LANES)
            row_y = (plane + lax.rem(cy + dy + part, SIDE)) * SIDE
            scores = dot(keys, q)
            for i in range(SIDE):
                key_nat = natural(late_k, row_y + lax.rem(cx + i, SIDE)) + u
                visible = (key_nat >= row_first) & (key_nat <= row_nat)
                rows = slice(i * ROWS, (i + 1) * ROWS)
                for l in range(SIDE):
                    tile = jnp.where(visible, scores[rows, l * LANES:(l + 1) * LANES], NEG_BIG)
                    gacc[rows, span(SCORE_BUFS[buf] + part * QL + l * LANES)] = tile
                    for r in range(0, ROWS, SUBLANES):
                        tops[l] = jnp.maximum(tops[l], tile[r:r + SUBLANES])
        mx[buf] = jnp.concatenate(tops, axis=1)

    def soften(s, buf):
        late_q, _, _, dy, lanes = step(s)
        qh = late_q.astype(jnp.int32)
        m_old = ml[qh, 0, :1]
        m_new = jnp.maximum(m_old, jnp.max(mx[buf], axis=0, keepdims=True))
        shift = m_new * EXP_SCALE
        p = jnp.concatenate([jnp.exp2(gacc[:, span(SCORE_BUFS[buf] + i * QL, QL)] * EXP_SCALE - shift) for i in BOTH], axis=0)
        alpha = jnp.exp2((m_old - m_new) * EXP_SCALE)
        ml[qh, 0, :1] = m_new
        ml[qh, 1, :1] = ml[qh, 1, :1] * alpha + jnp.sum(p, axis=0, keepdims=True)
        vals = w1[K_SLOT + 1, pl.ds(dy, 2), :, :, lanes].reshape(2 * SIDE * ROWS, LANES)
        pv = lax.dot_general(vals, p.astype(BF16), (((0,), (0,)), ((), ())), preferred_element_type=F32)
        acc[qh, :, :QL] = acc[qh, :, :QL] * alpha + pv

    product(0, 0)

    @pl.loop(0, STEPS // 2)
    def _(i):
        @pl.when(i == NEAR // 2)
        def _():
            all_there()
            product(NEAR, 0)

        product(2 * i + 1, 1)
        soften(2 * i, 0)
        product(jnp.where((i == NEAR // 2 - 1) | (i == STEPS // 2 - 1), 0, 2 * i + 2), 0)
        soften(2 * i + 1, 1)

    for hp in range(PAIR_HEADS):
        for half, rows in enumerate((EARLY, LATE)):
            o = (acc[half, :, span(hp * LANES)] / ml[half, 1, :1, span(hp * LANES)]).T.astype(BF16)
            for u in BOTH:
                for i, r in enumerate(rows):
                    obuf[core, r, span((2 * hp + u) * LANES)] = o[ROWS * u + CHUNK * i:ROWS * u + CHUNK * (i + 1)]
    o_copy = to_sib(obuf.at[core], obuf.at[core], os_sem, or_sem)
    o_copy.start()
    each(range(len(SENDS)), 'send', sent)
    for n in range(K_SLOT, N1):
        w1_start(n)

    def o_part(n, own):
        group = core if own else other
        places = BOTH if own else range(2, O_WIDE)
        slots = [w2_wait(Q_TRIPS + O_WIDE * n + u) for u in places]

        def part(cols):
            terms = [dot(obuf[group, :, u % 2 * KC:(u % 2 + 1) * KC], w2[s, :, :, :, cols].reshape(KC, QL)) for u, s in zip(places, slots)]
            if not own:
                for h in BOTH:
                    w = bbuf[:, span((2 * n + h) * NB + cols.start, QL)]
                    terms.append(dot(obuf[group, :, span(KC + h * PAIR * 2, PAIR * 2)], w))
            return sum(terms)

        return part

    def o_block(n, parts):
        total = jnp.zeros((PAIR, LANES), F32)
        for h in BOTH:
            o_spare(n, h).wait()
        for b in range(0, NB, QL):
            out = sum(p(slice(b, b + QL)) for p in parts)
            cols = span(own_col(n * NB) + b, QL)
            h = (x128[:, cols].astype(F32) + out).astype(BF16)
            x128[:, cols] = h
            hf = h.astype(F32)
            for u in range(0, QL, LANES):
                total = total + hf[:, u:u + LANES] * hf[:, u:u + LANES]
        ss[core] += total
        for u in range(O_WIDE):
            w2_start(Q_TRIPS + O_WIDE * n + u + N2)

    ss[core] = jnp.zeros((PAIR, LANES), F32)
    first = o_part(0, True)
    for b in range(0, NB, QL):
        acc[0, :, b:b + QL] = first(slice(b, b + QL))
    o_copy.wait()
    o_block(0, [lambda cols: acc[0, :, cols], o_part(0, False)])

    @pl.loop(1, BLOCKS_N)
    def _(n):
        o_block(n, [o_part(n, True), o_part(n, False)])

    for dim, k in NEIGHBOURS:
        for c in BOTH:
            pl.semaphore_signal(free_sem, device_id={'cp': peer(dim, SIDE - k, c)}, device_id_type=MESH)
    ss_copy = to_sib(ss.at[core], ss.at[core], sss_sem, ssr_sem)
    ss_copy.start()
    gacc[...] = jnp.zeros_like(gacc)
    acc[...] = jnp.zeros_like(acc)
    ss_copy.wait()
    inv_h = lax.rsqrt(jnp.sum(ss[0] + ss[1], axis=1, keepdims=True) / MODEL + NORM_EPS)

    def b_copy(i, col=own_col):
        part = bbuf.at[pair_rows, span(col(i * BC), BC)]
        return to_sib(part, part, bs_sem.at[i], br_sem.at[i])

    def n_copy(cross, i, g):
        dim, k = NEIGHBOURS[g]
        cols = span(own_col(i * BC), BC)
        return remote(bbuf.at[pl.ds(g * GROUP, GROUP), cols], bbuf.at[pl.ds(PAIR + g * GROUP, GROUP), cols],
                      ns_sem.at[cross, i, g], nr_sem.at[cross, i, g], peer(dim, k, other if cross else core))

    def n_arrival(cross, i, g):
        dim, k = NEIGHBOURS[g]
        dst = bbuf.at[pl.ds(PAIR + g * GROUP, GROUP), span((sib_col if cross else own_col)(i * BC), BC)]
        return remote(dst, dst, ns_sem.at[cross, i, g], nr_sem.at[cross, i, g], peer(dim, SIDE - k, other if cross else core))

    pl.semaphore_wait(free_sem, 2 * len(NEIGHBOURS))

    @pl.loop(0, BP)
    def _(i):
        for j in range(BC // LANES):
            tile = lax.div(own_col(i * BC), LANES) + j
            cols = span(tile * LANES)
            bbuf[pair_rows, cols] = (x128[:, cols].astype(F32) * inv_h * gains[1, pl.ds(tile, 1), :]).astype(BF16)
        for g in GROUPS:
            n_copy(0, i, g).start()
        b_copy(i).start()

    @pl.loop(0, BP)
    def _(i):
        for g in GROUPS:
            n_copy(1, i, g).start()

    def h_copy(g):
        dim, k = NEIGHBOURS[g]
        rows = pl.ds(g * GROUP, GROUP)
        return remote(x128.at[rows, span(other_color * HALF + core * QUARTER, QUARTER)], x128.at[rows, span(other_color * HALF + other * QUARTER, QUARTER)],
                      hs_sem.at[g], hr_sem.at[g], peer(dim, k))

    def h_arrival(g):
        dim, k = NEIGHBOURS[g]
        dst = x128.at[pl.ds(g * GROUP, GROUP), span(color * HALF + other * QUARTER, QUARTER)]
        return remote(dst, dst, hs_sem.at[g], hr_sem.at[g], peer(dim, SIDE - k))

    for g in GROUPS:
        h_copy(g).start()

    def narrow_part(s):
        return lambda i, cols: w1[s, 2 * i:2 * i + 2, :, :, cols]

    def gate_up(rows, t, weights):
        parts = [(bbuf[rows, span(g_cols(t) + u * KC, KC)], w) for u, w in enumerate(weights)]

        def block(i, cols):
            return [w(i, cols).reshape(KC, cols.stop - cols.start) for _, w in parts]

        def product_of(weights):
            return sum(dot(a, w) for (a, _), w in zip(parts, weights))

        for i in BOTH:
            for b in range(0, FFQ - LANES, QL):
                gacc[rows, i * FFQ + b:i * FFQ + b + QL] += product_of(block(i, slice(b, b + QL)))
        last = slice(FFQ - LANES, FFQ)
        pair = product_of([jnp.concatenate(w, axis=1) for w in zip(block(0, last), block(1, last))])
        gacc[rows, last] += pair[:, :LANES]
        gacc[rows, 2 * FFQ - LANES:] += pair[:, LANES:]

    def refill(t):
        for u in BOTH:
            w1_start(2 * t + u + N1)

    @pl.loop(0, PRE)
    def _(t):
        gate_up(slice(0, PAIR), t, [narrow_part(w1_wait(2 * t + u)) for u in BOTH])

    @pl.loop(0, PRE)
    def _(t):
        for g in GROUPS:
            n_arrival(0, t, g).wait_recv()
        gate_up(slice(PAIR, 2 * PAIR), t, [narrow_part(2 * t + u) for u in BOTH])
        refill(t)

    def wide_part(n):
        slots = [(n + i) % N2 for i in BOTH]
        for slot in slots:
            dst = w2.at[slot, :, :, :, pl.ds(0, FFQ)]
            pltpu.make_async_copy(wg.at[w_rows(0), :, :, span(0, FFQ)], dst, w2_sem.at[slot]).wait()
        return lambda i, cols: w2[slots[i], :, :, :, cols]

    for g in GROUPS:
        n_arrival(0, PRE, g).wait_recv()
    gate_up(slice(0, 2 * PAIR), PRE, [wide_part(WIDE_G + 2 * u) for u in BOTH])

    @pl.loop(PRE + 1, G_TRIPS)
    def _(t):
        @pl.when(t < BP)
        def _():
            for g in GROUPS:
                n_arrival(0, t, g).wait_recv()

        @pl.when(t >= BP)
        def _():
            b_copy(t - BP, sib_col).wait_recv()
            for g in GROUPS:
                n_arrival(1, t - BP, g).wait_recv()

        gate_up(slice(0, 2 * PAIR), t, [narrow_part(w1_wait(2 * t - 2 + u)) for u in BOTH])
        refill(t - 1)

        @pl.when(t == G_TRIPS - 2)
        def _():
            for n in range(WIDE_LATE, WIDE_LATE + D_LATE + 1):
                w2_start(n)

    def gated(rows):
        @pl.loop(0, FFQ // LANES)
        def _(j):
            g = gacc[rows, span(j * LANES)]
            mbuf[rows, span(hidden + j * LANES)] = (g * (1.0 / (1.0 + jnp.exp(-g))) * gacc[rows, span(FFQ + j * LANES)]).astype(BF16)

    def kind_rows(kind, g):
        return pl.ds(kind * PAIR + g * GROUP, GROUP)

    def m_send(kind, cross, g):
        dim, k = NEIGHBOURS[g]
        cols = span(hidden, FFQ)
        return remote(mbuf.at[kind_rows(kind, g), cols], mbuf.at[kind_rows(1 - kind, g), cols], nms_sem.at[kind, cross, g],
                      nmr_sem.at[1 - kind, cross, g], peer(dim, k if kind == 0 else SIDE - k, other if cross else core))

    def m_place(kind, g, c):
        return mbuf.at[kind_rows(kind, g), span(other_color * FFH + c * FFQ, FFQ)]

    def m_arrival(kind, cross, g):
        dim, k = NEIGHBOURS[g]
        dst = m_place(kind, g, other if cross else core)
        return remote(dst, dst, nms_sem.at[kind, cross, g], nmr_sem.at[kind, cross, g], peer(dim, k if kind == 0 else SIDE - k))

    def m_pass_on(g, c=core):
        part = m_place(0, g, c)
        return to_sib(part, part, fms_sem.at[g], fmr_sem.at[g])

    def m_copy(of_core):
        part = mbuf.at[:, span(color * FFH + of_core * FFQ, FFQ)]
        return to_sib(part, part, ms_sem, mr_sem)

    for kind in BOTH:
        gated(pl.ds(kind * PAIR, PAIR))
        for cross in range(2 - kind):
            for g in GROUPS:
                m_send(kind, cross, g).start()
    m_copy(core).start()

    def d_rows(rows, kk):
        return mbuf[rows, span(d_chunk(kk) * KC, KC)]

    def first_product(kk, weights):
        a = d_rows(slice(0, 2 * PAIR), kk)
        for n, weight in enumerate(weights):
            for b in range(0, NB, QL):
                out = dot(a, weight(slice(b, b + QL)))
                for r in BOTH:
                    acc[2 * n + r, :, b:b + QL] += out[r * PAIR:(r + 1) * PAIR]

    def of_wide(slot):
        return lambda cols: w2[slot, :, :, :, cols].reshape(KC, QL)

    def of_narrow(slot):
        return lambda cols: w1[slot, cols.start // BC * 2:cols.start // BC * 2 + 2, :, :, cols.start % BC:cols.start % BC + QL].reshape(KC, QL)

    @pl.loop(0, SIDE)
    def _(kk):
        @pl.when(kk == 2)
        def _():
            m_copy(core).wait_send()
            m_copy(other).wait_recv()

        places = [d_wide(2 * kk + u) for u in BOTH]
        first_product(kk, [of_wide(w2_wait(n)) for n in places])
        for n in places:
            w2_start(n + N2)

    for kk in range(SIDE, D_OWN):
        places = [G_NARROW + 2 * (kk - SIDE) + u for u in BOTH]
        first_product(kk, [of_narrow(w1_wait_down(n)) for n in places])
        for n in places:
            if n + N1 < G_NARROW + len(D_NARROW):
                w1_start(n + N1)

    @pl.loop(0, BP)
    def _(i):
        b_copy(i).wait_send()
        for cross in BOTH:
            for g in GROUPS:
                n_copy(cross, i, g).wait_send()

    for cross in BOTH:
        for g in GROUPS:
            m_arrival(1, cross, g).wait_recv()
    for g in GROUPS:
        h_copy(g).wait_send()
        h_arrival(g).wait_recv()

    def d_slots(n, wait):
        found = []
        for i in range(D_FIRST + n * D_REST, D_FIRST + (n + 1) * D_REST):
            if i not in D_NARROW:
                place = d_wide(i)
                found.append((i, w2, place % N2))
                if wait:
                    w2_wait(place)
            else:
                place = G_NARROW + D_NARROW.index(i)
                found.append((i, w1, place % N1))
                if wait:
                    w1_wait_down(place)
        return found

    def d_cols(n, h, to_core=core, of_color=color):
        return span(of_color * HALF + to_core * QUARTER + n * NB + h * BC, BC)

    def second_product(kind, n, h, found):
        for b in range(0, BC, QL):
            out = acc[2 * n + kind, :, span(h * BC + b, QL)]
            for i, ring, slot in found:
                if ring is w2:
                    weight = w2[slot, :, :, :, span(h * BC + b, QL)]
                else:
                    weight = w1[slot, pl.ds(2 * h, 2), :, :, b:b + QL]
                out += dot(d_rows(pl.ds(kind * PAIR, PAIR), d_place(i)[1]), weight.reshape(KC, QL))
            place = n * NB + h * BC + b
            residual = x128[:, span(color * HALF + (other if kind else core) * QUARTER + place, QL)]
            bbuf[pl.ds(kind * PAIR, PAIR), span(color * HALF + core * QUARTER + place, QL)] = (residual.astype(F32) + out).astype(BF16)

    def z_away(n, h, g):
        dim, k = NEIGHBOURS[g]
        dst = z_hbm.at[pl.ds(g % 2 * GROUP, GROUP), d_cols(n, h)]
        return remote(bbuf.at[kind_rows(1, g), d_cols(n, h)], dst, za_sem.at[n, h, g], zb_sem.at[core, n, h, g % 2], peer(dim, SIDE - k, g // 2))

    def z_back(c, n, h, i):
        part = z_hbm.at[pl.ds(i * GROUP, GROUP), d_cols(n, h, c, other_color)]
        return to_sib(part, part, za_sem.at[n, h, i], zb_sem.at[c, n, h, i])

    def z_local(n, h):
        return pltpu.make_async_copy(bbuf.at[own_rows, d_cols(n, h)], z_hbm.at[:, d_cols(n, h)], zl_sem.at[n, h])

    def z_remote(n, h, c=core):
        return to_sib(bbuf.at[sib_rows, d_cols(n, h, c)], z_hbm.at[:, d_cols(n, h, c)], zs_sem.at[n, h], zr_sem.at[n, h])

    for n in range(D_BLOCKS):
        found = d_slots(n, True)

        @pl.loop(0, 2)
        def _(h):
            second_product(1, n, h, found)
            for g in GROUPS:
                z_away(n, h, g).start()

        if n == 0:
            for g in GROUPS:
                m_arrival(0, 0, g).wait_recv()
                m_pass_on(g).start()

    for g in GROUPS:
        m_pass_on(g).wait_send()
        m_pass_on(g, other).wait_recv()

    for n in range(D_BLOCKS):
        found = d_slots(n, False)

        @pl.loop(0, 2)
        def _(h):
            second_product(0, n, h, found)
            z_local(n, h).start()
            z_remote(n, h).start()

    for n in range(D_BLOCKS):
        for h in BOTH:
            z_local(n, h).wait()
            z_remote(n, h).wait_send()
            z_remote(n, h, other).wait_recv()
            for g in GROUPS:
                z_away(n, h, g).wait_send()
            for c in BOTH:
                for i in BOTH:
                    z_back(c, n, h, i).wait_recv()
    for kind in BOTH:
        for cross in range(2 - kind):
            for g in GROUPS:
                m_send(kind, cross, g).wait_send()
    for s in stores:
        s.wait()


def deliver_kernel(z_in, k_in, v_in, z_out, k_out, v_out, zb, kb, in_sem, out_sem):
    moves = [(k_in, kb.at[0], k_out), (v_in, kb.at[1], v_out)]
    for first in range(0, MODEL, DELIVER):
        cols = span(first, DELIVER)
        moves.append((z_in.at[:, cols], zb.at[:, cols], z_out.at[:, cols]))
    moves = [(pltpu.make_async_copy(src, mid, in_sem.at[i]), pltpu.make_async_copy(mid, dst, out_sem.at[i])) for i, (src, mid, dst) in enumerate(moves)]
    for come, _ in moves:
        come.start()
    for come, go in moves:
        come.wait()
        go.start()
    for _, go in moves:
        go.wait()


def solution(mesh):
    def device_fn(x_loc, seg_loc, pos_loc, attn_gain, w_q, w_k, w_v, w_o, mlp_gain, w_gate, w_up, w_down):
        any_space = pl.BlockSpec(memory_space=pl.ANY)
        vmem = pl.BlockSpec(memory_space=pltpu.VMEM)

        def blocks(w):
            return w.reshape(-1, SIDE, ROWS, w.shape[1])

        def gain(g):
            return g.reshape(-1, LANES)

        z_shape, k_shape = (jax.ShapeDtypeStruct((ROWS, n), BF16) for n in (MODEL, HEAD_DIM))
        outs = (z_shape, k_shape, k_shape)
        f32_buffers = ((BLOCKS_N, PAIR, NB), (2 * PAIR, 2 * FFQ))
        stats = ((2, 2, SUBLANES, QL), (2, SUBLANES, QL))
        sems = {
            'xl': (), 'xs': (XP,), 'xr': (XP,), 'sts': (), 'str': (), 'kvw': (2, KV_PIECES), 'w1': (N1,), 'w2': (N2,),
            'gs': (len(BLOCKS), len(SENDS), len(STEPS_ALONG)), 'gr': (len(BLOCKS), len(SENDS), len(STEPS_ALONG)),
            'fs': (len(BLOCKS), len(SENDS) + 1, len(STEPS_ALONG)), 'fr': (len(BLOCKS), len(SENDS) + 1, len(STEPS_ALONG)),
            'os': (), 'or': (), 'sss': (), 'ssr': (), 'bs': (BP,), 'br': (BP,), 'ns': (2, BP, len(GROUPS)), 'nr': (2, BP, len(GROUPS)),
            'ms': (), 'mr': (), 'nms': (2, 2, len(GROUPS)), 'nmr': (2, 2, len(GROUPS)), 'fms': (len(GROUPS),), 'fmr': (len(GROUPS),), 'hs': (len(GROUPS),), 'hr': (len(GROUPS),),
            'za': (D_BLOCKS, 2, len(GROUPS)), 'zb': (2, D_BLOCKS, 2, 2), 'zl': (D_BLOCKS, 2), 'zs': (D_BLOCKS, 2), 'zr': (D_BLOCKS, 2), 'ko': (2,), 'spare': (BLOCKS_N, 2),
        }

        def dma(shape):
            return pltpu.SemaphoreType.DMA(shape) if shape else pltpu.SemaphoreType.DMA

        results = pl.pallas_call(
            layer_kernel,
            out_shape=outs,
            in_specs=[any_space, vmem, vmem, any_space, any_space, any_space, any_space, any_space, vmem, any_space, any_space, any_space],
            out_specs=(any_space,) * len(outs),
            scratch_shapes=[
                pltpu.VMEM((PAIR, MODEL), BF16),
                pltpu.VMEM((2 * PAIR, MODEL), BF16),
                pltpu.VMEM((N1, SIDE, SIDE, ROWS, FFQ), BF16),
                pltpu.VMEM((N2, 2, SIDE, ROWS, NB), BF16),
                *(pltpu.VMEM(s, F32) for s in f32_buffers),
                pltpu.VMEM((2, HEAD_DIM, QL), BF16),
                *(pltpu.VMEM(s, F32) for s in stats),
                pltpu.VMEM((2, PAIR, QCOLS), BF16),
                pltpu.VMEM((2 * PAIR, FF), BF16),
                pltpu.VMEM((2, ROWS, LANES), F32),
                pltpu.VMEM((2, PAIR, LANES), F32),
                pltpu.VMEM((2, ROWS, LANES), BF16),
                pltpu.VMEM((2, LANES, LANES), F32),
                *(dma(s) for s in sems.values()),
                pltpu.SemaphoreType.REGULAR,
            ],
            compiler_params=pltpu.CompilerParams(collective_id=0, has_side_effects=True, vmem_limit_bytes=67043328),
            name='layer',
        )(x_loc[0], pos_loc.reshape(1, ROWS), gain(attn_gain), blocks(w_q), blocks(w_k), blocks(w_v), blocks(w_o), w_o, gain(mlp_gain),
          blocks(w_gate), blocks(w_up), blocks(w_down))
        moves = MODEL // DELIVER + 2
        z_rows, k_rows, v_rows = pl.pallas_call(
            deliver_kernel,
            out_shape=outs,
            in_specs=[any_space] * len(outs),
            out_specs=(any_space,) * len(outs),
            scratch_shapes=[pltpu.VMEM((ROWS, MODEL), BF16), pltpu.VMEM((2, ROWS, HEAD_DIM), BF16), dma((moves,)), dma((moves,))],
            compiler_params=pltpu.CompilerParams(vmem_limit_bytes=62914560),
            name='finish',
        )(*results)
        return z_rows[None], k_rows[:, None, :], v_rows[:, None, :]

    seq_spec = P(('dp', 'cp'))
    rows_spec, cache_spec = P('dp', 'cp', None), P(('dp', 'cp'), None, None)
    return jax.shard_map(device_fn, mesh=mesh, in_specs=(rows_spec, seq_spec, seq_spec) + (P(),) * 9, out_specs=(rows_spec, cache_spec, cache_spec), check_vma=False)
```
